128 devices in a mesh: dp: 1, sp: 64 (over z, y, x), tp: 2 (over core).
Axes of the slice: x: 4, y: 4, z: 4, core: 2. Of those that a mesh axis runs over, the one named last changes fastest.
Arguments:
- x_in: bfloat16 [16, 3072, 56, 64], P('dp', 'sp', None, 'tp')
- act_saved: bfloat16 [16, 3072, 56, 64], P('dp', 'sp', None, 'tp')
- w_one: bfloat16 [3, 3, 64, 64], P(None, None, 'tp')
- w_two: bfloat16 [3, 3, 64, 64], P(None, None, 'tp')
- d_out: bfloat16 [16, 3072, 56, 64], P('dp', 'sp', None, 'tp')
Outputs:
- output 1: bfloat16 [16, 3072, 56, 64], P('dp', 'sp', None, 'tp')
- output 2: float32 [3, 3, 64, 64], P('dp', None, 'tp')
- output 3: float32 [3, 3, 64, 64], P('dp', None, 'tp')
- output 4: float32 [64], P(('dp', 'tp'))
All inputs are finite; a program needn't handle non-finite values.
Results may differ from the reference program's by a relative error of at most 0.001.
Values are sent between devices in bfloat16 or wider.
A program may use at most 1 GiB of HBM per device.

```python
import jax
import jax.numpy as jnp
from jax import lax

BATCH_SIZE = 16
HEIGHT = 3072
IMG_WIDTH = 56
CHANNELS = 64


def setup_inputs(seed: int = 0, part: int = 0) -> dict:
    part_key = jax.random.fold_in(jax.random.key(seed), part)
    key_list = jax.random.split(part_key, 3)
    shared_list = jax.random.split(jax.random.key(seed + 1), 2)
    arr_shape = (BATCH_SIZE, HEIGHT, IMG_WIDTH, CHANNELS)
    kern_shape = (3, 3, CHANNELS, CHANNELS)
    kern_scale = (9 * CHANNELS) ** -0.5
    x_in = jax.random.normal(key_list[0], arr_shape, jnp.float32).astype(jnp.bfloat16)
    act_saved = jnp.maximum(jax.random.normal(key_list[1], arr_shape, jnp.float32), 0.0).astype(jnp.bfloat16)
    d_out = jax.random.normal(key_list[2], arr_shape, jnp.float32).astype(jnp.bfloat16)
    w_one = (jax.random.normal(shared_list[0], kern_shape, jnp.float32) * kern_scale).astype(jnp.bfloat16)
    w_two = (jax.random.normal(shared_list[1], kern_shape, jnp.float32) * kern_scale).astype(jnp.bfloat16)
    return {"x_in": x_in, "act_saved": act_saved, "w_one": w_one, "w_two": w_two, "d_out": d_out}


def conv_forward(image, kernel):
    return lax.conv_general_dilated(image, kernel, (1, 1), "SAME", dimension_numbers=("NHWC", "HWIO", "NHWC"))


def reference(x_in, act_saved, w_one, w_two, d_out):
    cot_out = d_out.astype(jnp.float32)
    pull_two = jax.vjp(conv_forward, act_saved.astype(jnp.float32), w_two.astype(jnp.float32))[1]
    d_act, grad_two = pull_two(cot_out)
    masked = jnp.where(act_saved > 0, d_act, 0.0)
    grad_bias = jnp.sum(masked, axis=(0, 1, 2))
    d_pre = masked.astype(jnp.bfloat16).astype(jnp.float32)
    pull_one = jax.vjp(conv_forward, x_in.astype(jnp.float32), w_one.astype(jnp.float32))[1]
    d_conv, grad_one = pull_one(d_pre)
    d_x = (cot_out + d_conv).astype(jnp.bfloat16)
    return d_x, grad_one, grad_two, grad_bias
```

```python
import functools

import jax
import jax.numpy as jnp
from jax import lax
from jax.experimental import pallas as pl
from jax.experimental.pallas import tpu as pltpu
from jax.sharding import PartitionSpec as P

MESH = pl.DeviceIdType.MESH
BF16 = jnp.bfloat16
F32 = jnp.float32


def body(side, rows, chunk, x_hbm, a_hbm, g_hbm, w_one, w_two, dx_hbm, dw_one, dw_two, dbias,
         raw_g, raw_a, raw_x, g_all, z_all, a_pk, x_pk, wm_one, wm_two, acc, bacc, red,
         load_sem, out_sem, gx_send, gx_recv, gh_send, gh_recv, zx_send, zx_recv, zh_send, zh_recv,
         ar_send, ar_recv):
    sp = lax.axis_index("sp")
    tp = lax.axis_index("tp")
    row_devs = side * side * side
    n_chunks = rows // chunk
    n_blocks = rows // 2
    coords = (lax.rem(sp, side), lax.rem(lax.div(sp, side), side), lax.div(sp, side * side))
    strides = (1, side, side * side)
    nxt = lax.rem(sp + 1, row_devs)
    prv = lax.rem(sp + row_devs - 1, row_devs)
    other = 1 - tp
    mine = pl.ds(pl.multiple_of(tp * 32, 32), 32)
    theirs = pl.ds(pl.multiple_of(other * 32, 32), 32)

    def ring_peer(axis, k):
        me = coords[axis]
        return sp + (lax.rem(me + k, side) - me) * strides[axis]

    order = [0] + ([n_chunks - 1] if n_chunks > 1 else []) + list(range(1, n_chunks - 1))

    def load(i, c):
        src = (g_hbm, a_hbm, x_hbm)[i]
        dst = (raw_g, raw_a, raw_x)[i]
        return pltpu.make_async_copy(src.at[:, pl.ds(c * chunk, chunk)], dst.at[:, pl.ds(c * chunk, chunk)], load_sem.at[i, c])

    for i in range(3):
        for c in order:
            load(i, c).start()

    barrier = pltpu.get_barrier_semaphore()
    targets = [(sp, other), (nxt, tp), (nxt, other), (prv, tp), (prv, other)]
    for axis in range(3):
        for k in range(1, side):
            targets.append((ring_peer(axis, k), tp))
    for s, t in targets:
        pl.semaphore_signal(barrier, inc=1, device_id={"sp": s, "tp": t}, device_id_type=MESH)

    for w_ref, wm in ((w_two, wm_two), (w_one, wm_one)):
        wm[...] = jnp.zeros_like(wm)
        for kw in range(3):
            for r in range(2):
                blocks = []
                for rr in range(4):
                    kh = r + 2 - rr
                    blocks.append(w_ref[kh, kw] if 0 <= kh < 3 else jnp.zeros((32, 64), BF16))
                wm[pl.ds(kw * 64 + r * 32, 32), :] = jnp.concatenate(blocks, axis=1)

    def pack(raw, dst, lo, off, sl):
        def step(h, carry):
            for j in range(8):
                left = raw[j, h]
                right = raw[j + 8, h]
                gap = jnp.zeros((32, 8), BF16)
                dst[h + off, sl, pl.ds(j * 128, 128)] = jnp.concatenate([left, gap, right, gap], axis=1)
            return carry
        lax.fori_loop(lo, lo + chunk, step, 0)

    def remote(ref, idx, send, recv, s, t):
        return pltpu.make_async_remote_copy(src_ref=ref.at[idx], dst_ref=ref.at[idx], send_sem=send, recv_sem=recv,
                                            device_id={"sp": s, "tp": t}, device_id_type=MESH)

    def pair(ref, lo, n, send, recv, sl):
        return remote(ref, (pl.ds(lo, n), sl), send, recv, sp, other)

    def halo(ref, up, rel, send, recv):
        src_row, dst_row, dev = (rows, 0, nxt) if up == 0 else (1, rows + 1, prv)
        return pltpu.make_async_remote_copy(
            src_ref=ref.at[src_row, mine], dst_ref=ref.at[dst_row, mine], send_sem=send.at[up, rel], recv_sem=recv.at[up, rel],
            device_id={"sp": dev, "tp": tp if rel == 0 else other}, device_id_type=MESH)

    def halo_wait(ref, up, rel, send, recv):
        dst_row, dev = (0, prv) if up == 0 else (rows + 1, nxt)
        sl = mine if rel == 0 else theirs
        pltpu.make_async_remote_copy(
            src_ref=ref.at[dst_row, sl], dst_ref=ref.at[dst_row, sl], send_sem=send.at[up, rel], recv_sem=recv.at[up, rel],
            device_id={"sp": dev, "tp": tp if rel == 0 else other}, device_id_type=MESH).wait_recv()

    def halo_finish(ref, send, recv):
        for up in range(2):
            for rel in range(2):
                halo_wait(ref, up, rel, send, recv)

        @pl.when(sp == 0)
        def _():
            ref[0] = jnp.zeros((64, 1024), BF16)

        @pl.when(sp == row_devs - 1)
        def _():
            ref[rows + 1] = jnp.zeros((64, 1024), BF16)

    first = True
    for c in order:
        load(0, c).wait()
        pack(raw_g, g_all, c * chunk, 1, mine)
        if first:
            pl.semaphore_wait(barrier, len(targets))
            first = False
        if c == 0:
            for rel in range(2):
                halo(g_all, 1, rel, gh_send, gh_recv).start()
        if c == n_chunks - 1:
            for rel in range(2):
                halo(g_all, 0, rel, gh_send, gh_recv).start()
        pair(g_all, c * chunk + 1, chunk, gx_send.at[c], gx_recv.at[c], mine).start()

    for c in order:
        load(1, c).wait()
        pack(raw_a, a_pk, c * chunk, 0, slice(None))
    bacc[...] = jnp.zeros_like(bacc)
    acc[...] = jnp.zeros_like(acc)
    for c in order:
        pair(g_all, c * chunk + 1, chunk, gx_send.at[c], gx_recv.at[c], theirs).wait_recv()
    halo_finish(g_all, gh_send, gh_recv)

    def conv_tile(src, wm, b, q):
        tile = src[pl.ds(2 * b, 4), :, pl.ds(q * 256, 256)].reshape(256, 256)
        d = jnp.dot(wm[...], tile, preferred_element_type=F32)
        outs = []
        for s in range(2):
            part = d[:, s * 128:(s + 1) * 128]
            outs.append(part[64:128] + pltpu.roll(part[0:64], 127, 1) + pltpu.roll(part[128:192], 1, 1))
        return outs

    def dz_block(b):
        for q in range(4):
            for s, o in enumerate(conv_tile(g_all, wm_two, b, q)):
                lanes = pl.ds(q * 256 + s * 128, 128)
                av = a_pk[pl.ds(2 * b, 2), :, lanes].reshape(64, 128).astype(F32)
                m = jnp.where(av > 0, o, 0.0)
                bacc[...] += m
                z = m.astype(BF16)
                z_all[2 * b + 1, mine, lanes] = z[0:32]
                z_all[2 * b + 2, mine, lanes] = z[32:64]

    groups = [(0, 1), (n_blocks - 1, 1)]
    inner = n_blocks - 2
    lo = 1
    for i in range(4):
        n = inner // 4 + (1 if i < inner % 4 else 0)
        if n:
            groups.append((lo, n))
            lo += n
    for gi, (lo, n) in enumerate(groups):
        if n == 1:
            dz_block(lo)
        else:
            lax.fori_loop(lo, lo + n, lambda b, _: (dz_block(b), 0)[1], 0)
        if lo == 0:
            for rel in range(2):
                halo(z_all, 1, rel, zh_send, zh_recv).start()
        if lo + n == n_blocks:
            for rel in range(2):
                halo(z_all, 0, rel, zh_send, zh_recv).start()
        pair(z_all, 2 * lo + 1, 2 * n, zx_send.at[gi], zx_recv.at[gi], mine).start()

    def wgrad(src, gref):
        def step(b, carry):
            cur = src[pl.ds(2 * b, 2)].reshape(64, 1024)
            tiles = [cur[:, j * 128:(j + 1) * 128] for j in range(8)]
            left = jnp.concatenate([pltpu.roll(t, 1, 1) for t in tiles], axis=1)
            right = jnp.concatenate([pltpu.roll(t, 127, 1) for t in tiles], axis=1)
            lhs = jnp.concatenate([left, cur, right], axis=0)
            rhs = gref[pl.ds(2 * b, 4)].reshape(256, 1024)
            acc[...] += lax.dot_general(lhs, rhs, (((1,), (1,)), ((), ())), preferred_element_type=F32)
            return carry
        lax.fori_loop(0, n_blocks, step, 0)

    def reduce_copy(i, p, t, k, slot):
        axis = (p + t) % 3
        ref = red.at[i, p, t, slot]
        return pltpu.make_async_remote_copy(src_ref=ref, dst_ref=ref, send_sem=ar_send.at[i, p, t, k - 1], recv_sem=ar_recv.at[i, p, t, k - 1],
                                            device_id={"sp": ring_peer(axis, k), "tp": tp}, device_id_type=MESH)

    def reduce_start(i, p):
        for t in range(3):
            for k in range(1, side):
                reduce_copy(i, p, t, k, coords[(p + t) % 3]).start()

    def reduce_begin(i, extra):
        for t in range(3):
            top = acc[pl.ds(t * 64, 32), :]
            low = acc[pl.ds(t * 64 + 32, 32), :]
            e = top[:, 0:192] + low[:, 64:256]
            tail = extra if t == 0 else jnp.zeros((32, 64), F32)
            red[i, 0, t, coords[t]] = jnp.concatenate([e, tail], axis=1)
        reduce_start(i, 0)

    def reduce_step(i, p):
        for t in range(3):
            axis = (p + t) % 3
            me = coords[axis]
            for k in range(1, side):
                reduce_copy(i, p, t, k, lax.rem(me - k + side, side)).wait_recv()
            total = red[i, p, t, 0]
            for c in range(1, side):
                total = total + red[i, p, t, c]
            if p < 2:
                red[i, p + 1, t, coords[(p + 1 + t) % 3]] = total
            else:
                out = (dw_one, dw_two)[i]
                for kh in range(3):
                    out[kh, t] = total[:, (2 - kh) * 64:(3 - kh) * 64]
                if i == 0 and t == 0:
                    wide = jnp.concatenate([total[:, 192:256], jnp.zeros((32, 64), F32)], axis=1)
                    dbias[...] = jnp.sum(wide.T, axis=0, keepdims=True)
        if p < 2:
            reduce_start(i, p + 1)

    wgrad(a_pk, g_all)
    reduce_begin(1, jnp.zeros((32, 64), F32))

    for c in order:
        load(2, c).wait()
        pack(raw_x, x_pk, c * chunk, 0, slice(None))
    acc[...] = jnp.zeros_like(acc)
    for gi, (lo, n) in enumerate(groups):
        pair(z_all, 2 * lo + 1, 2 * n, zx_send.at[gi], zx_recv.at[gi], theirs).wait_recv()
    halo_finish(z_all, zh_send, zh_recv)
    wgrad(x_pk, z_all)
    both = bacc[0:32, :] + bacc[32:64, :]
    reduce_begin(0, both[:, 0:64] + both[:, 64:128])
    reduce_step(1, 0)

    def dx_block(b):
        for q in range(4):
            for s, o in enumerate(conv_tile(z_all, wm_one, b, q)):
                j = 2 * q + s
                lanes = pl.ds(j * 128, 128)
                for r in range(2):
                    gy = g_all[2 * b + 1 + r, mine, lanes].astype(F32)
                    v = (gy + o[r * 32:(r + 1) * 32]).astype(BF16)
                    raw_g[j, 2 * b + r] = v[:, 0:56]
                    raw_g[j + 8, 2 * b + r] = v[:, 64:120]

    def store(c):
        return pltpu.make_async_copy(raw_g.at[:, pl.ds(c * chunk, chunk)], dx_hbm.at[:, pl.ds(c * chunk, chunk)], out_sem.at[c])

    marks = {n_chunks // 3: ((1, 1), (0, 0)), (2 * n_chunks) // 3: ((1, 2), (0, 1))}
    for c in range(n_chunks):
        for i, p in marks.get(c, ()):
            reduce_step(i, p)
        lax.fori_loop(c * chunk // 2, (c + 1) * chunk // 2, lambda b, _: (dx_block(b), 0)[1], 0)
        store(c).start()
    reduce_step(0, 2)

    for c in range(n_chunks):
        store(c).wait()
        pair(g_all, c * chunk + 1, chunk, gx_send.at[c], gx_recv.at[c], mine).wait_send()
    for gi, (lo, n) in enumerate(groups):
        pair(z_all, 2 * lo + 1, 2 * n, zx_send.at[gi], zx_recv.at[gi], mine).wait_send()
    for up in range(2):
        for rel in range(2):
            halo(g_all, up, rel, gh_send, gh_recv).wait_send()
            halo(z_all, up, rel, zh_send, zh_recv).wait_send()
    for i in range(2):
        for p in range(3):
            for t in range(3):
                for k in range(1, side):
                    reduce_copy(i, p, t, k, coords[(p + t) % 3]).wait_send()


def solution(mesh):
    side = round(mesh.shape["sp"] ** (1 / 3))

    def local_step(x_in, act_saved, w_one, w_two, d_out):
        swap = lambda v: jnp.transpose(v, (0, 1, 3, 2))
        imgs, rows, width, ch = x_in.shape
        chunk = 8 if rows % 8 == 0 else 2
        n_chunks = rows // chunk
        raw = pltpu.VMEM((imgs, rows, ch, width), BF16)
        full = pltpu.VMEM((rows + 2, 64, 1024), BF16)
        half = pltpu.VMEM((rows, 32, 1024), BF16)
        dma = pltpu.SemaphoreType.DMA
        n_groups = 6
        vmem = pl.BlockSpec(memory_space=pltpu.VMEM)
        hbm = pl.BlockSpec(memory_space=pl.ANY)
        dx, dw_one, dw_two, dbias = pl.pallas_call(
            functools.partial(body, side, rows, chunk),
            out_shape=(
                jax.ShapeDtypeStruct((imgs, rows, ch, width), BF16),
                jax.ShapeDtypeStruct((3, 3, 32, 64), F32),
                jax.ShapeDtypeStruct((3, 3, 32, 64), F32),
                jax.ShapeDtypeStruct((1, 32), F32),
            ),
            in_specs=[hbm, hbm, hbm, vmem, vmem],
            out_specs=(hbm, vmem, vmem, vmem),
            scratch_shapes=[
                raw, raw, raw, full, full, half, half,
                pltpu.VMEM((192, 256), BF16), pltpu.VMEM((192, 256), BF16),
                pltpu.VMEM((192, 256), F32), pltpu.VMEM((64, 128), F32),
                pltpu.VMEM((2, 3, 3, side, 32, 256), F32),
                dma((3, n_chunks)), dma((n_chunks,)),
                dma((n_chunks,)), dma((n_chunks,)), dma((2, 2)), dma((2, 2)),
                dma((n_groups,)), dma((n_groups,)), dma((2, 2)), dma((2, 2)),
                dma((2, 3, 3, side - 1)), dma((2, 3, 3, side - 1)),
            ],
            compiler_params=pltpu.CompilerParams(collective_id=0, has_side_effects=True, vmem_limit_bytes=60 * 1024 * 1024),
            name="resblock_bwd",
        )(swap(x_in), swap(act_saved), swap(d_out), w_one, w_two)
        return swap(dx), dw_one, dw_two, dbias.reshape(32)

    act_spec = P("dp", "sp", None, "tp")
    kern_spec = P(None, None, "tp", None)
    grad_spec = P("dp", None, "tp", None)
    return jax.shard_map(local_step, mesh=mesh, in_specs=(act_spec, act_spec, kern_spec, kern_spec, act_spec),
                         out_specs=(act_spec, grad_spec, grad_spec, P(("dp", "tp"))), check_vma=False)
```

```python
import functools

import jax
import jax.numpy as jnp
from jax import lax
from jax.experimental import pallas as pl
from jax.experimental.pallas import tpu as pltpu
from jax.sharding import PartitionSpec as P

MESH = pl.DeviceIdType.MESH
BF16 = jnp.bfloat16
F32 = jnp.float32


def body(side, rows, x_hbm, a_hbm, g_hbm, w_one, w_two, dx_hbm, dw_one, dw_two, dbias,
         raw_g, raw_a, raw_x, g_all, z_all, wm_one, wm_two, acc, bacc, red,
         g_sem, a_sem, x_sem, out_sem, gx_send, gx_recv, gh_send, gh_recv, zx_send, zx_recv, zh_send, zh_recv,
         ar_send, ar_recv):
    sp = lax.axis_index("sp")
    tp = lax.axis_index("tp")
    row_devs = side * side * side
    n_groups = rows // 8
    n_blocks = rows // 2
    coords = (lax.rem(sp, side), lax.rem(lax.div(sp, side), side), lax.div(sp, side * side))
    strides = (1, side, side * side)
    nxt = lax.rem(sp + 1, row_devs)
    prv = lax.rem(sp + row_devs - 1, row_devs)
    other = 1 - tp
    mine = pl.ds(pl.multiple_of(tp * 32, 32), 32)
    theirs = pl.ds(pl.multiple_of(other * 32, 32), 32)

    def ring_peer(axis, k):
        me = coords[axis]
        return sp + (lax.rem(me + k, side) - me) * strides[axis]

    def load_g(c):
        part = pl.ds(c * 8, 8)
        return pltpu.make_async_copy(g_hbm.at[:, part], raw_g.at[:, part], g_sem.at[c])

    load_a = pltpu.make_async_copy(a_hbm, raw_a, a_sem)
    load_x = pltpu.make_async_copy(x_hbm, raw_x, x_sem)

    for i in range(n_groups):
        load_g((i + n_groups - 1) % n_groups).start()

    barrier = pltpu.get_barrier_semaphore()
    targets = [(sp, other), (nxt, tp), (nxt, other), (prv, tp), (prv, other)]
    for axis in range(3):
        for k in range(1, side):
            targets.append((ring_peer(axis, k), tp))
    for s, t in targets:
        pl.semaphore_signal(barrier, inc=1, device_id={"sp": s, "tp": t}, device_id_type=MESH)
    load_a.start()

    for w_ref, wm in ((w_two, wm_two), (w_one, wm_one)):
        for kw in range(3):
            for r in range(2):
                blocks = []
                for rr in range(4):
                    kh = r + 2 - rr
                    blocks.append(w_ref[kh, kw] if 0 <= kh < 3 else jnp.zeros((32, 64), BF16))
                wm[pl.ds(kw * 64 + r * 32, 32), :] = jnp.concatenate(blocks, axis=1)
    bacc[...] = jnp.zeros_like(bacc)
    acc[...] = jnp.zeros_like(acc)

    def packed(raw, h, j):
        gap = jnp.zeros((32, 8), BF16)
        return jnp.concatenate([raw[j, h], gap, raw[j + 8, h], gap], axis=1)

    def remote(ref, lo, n, sl, send, recv):
        part = ref.at[pl.ds(lo, n), :, sl]
        return pltpu.make_async_remote_copy(src_ref=part, dst_ref=part, send_sem=send, recv_sem=recv,
                                            device_id={"sp": sp, "tp": other}, device_id_type=MESH)

    def halo(ref, up, rel, send, recv):
        src_row, dst_row, dev = (rows, 0, nxt) if up == 0 else (1, rows + 1, prv)
        return pltpu.make_async_remote_copy(
            src_ref=ref.at[src_row, :, mine], dst_ref=ref.at[dst_row, :, mine], send_sem=send.at[up, rel], recv_sem=recv.at[up, rel],
            device_id={"sp": dev, "tp": tp if rel == 0 else other}, device_id_type=MESH)

    def halo_finish(ref, send, recv):
        for up in range(2):
            for rel in range(2):
                dst_row, dev = (0, prv) if up == 0 else (rows + 1, nxt)
                part = ref.at[dst_row, :, mine if rel == 0 else theirs]
                pltpu.make_async_remote_copy(
                    src_ref=part, dst_ref=part, send_sem=send.at[up, rel], recv_sem=recv.at[up, rel],
                    device_id={"sp": dev, "tp": tp if rel == 0 else other}, device_id_type=MESH).wait_recv()

        @pl.when(sp == 0)
        def _():
            ref[0] = jnp.zeros((8, 64, 128), BF16)

        @pl.when(sp == row_devs - 1)
        def _():
            ref[rows + 1] = jnp.zeros((8, 64, 128), BF16)

    def g_pair(c, sl):
        return remote(g_all, c * 8 + 1, 8, sl, gx_send.at[c], gx_recv.at[c])

    def z_pair(g, part, sl):
        lo = lax.rem(8 * g + part * 4 + rows - 4, rows) + 1
        return remote(z_all, lo, 4, sl, zx_send.at[g, part], zx_recv.at[g, part])

    pl.semaphore_wait(barrier, len(targets))

    def pack_g(i, carry):
        c = lax.rem(i + n_groups - 1, n_groups)
        load_g(c).wait()
        for h in range(8):
            for j in range(8):
                g_all[c * 8 + h + 1, j, mine] = packed(raw_g, c * 8 + h, j)

        @pl.when(i == 0)
        def _():
            for rel in range(2):
                halo(g_all, 0, rel, gh_send, gh_recv).start()

        @pl.when(i == 1)
        def _():
            for rel in range(2):
                halo(g_all, 1, rel, gh_send, gh_recv).start()

        g_pair(c, mine).start()
        return carry

    lax.fori_loop(0, n_groups, pack_g, 0)
    load_x.start()

    def conv_tile(src, wm, b, q):
        tile = jnp.concatenate([src[pl.ds(2 * b, 4), 2 * q + s].reshape(256, 128) for s in range(2)], axis=1)
        d = jnp.dot(wm[...], tile, preferred_element_type=F32)
        outs = []
        for s in range(2):
            part = d[:, s * 128:(s + 1) * 128]
            outs.append(part[64:128] + pltpu.roll(part[0:64], 127, 1) + pltpu.roll(part[128:192], 1, 1))
        return outs

    def shifted(tiles):
        left = jnp.concatenate([pltpu.roll(t, 1, 1) for t in tiles], axis=1)
        right = jnp.concatenate([pltpu.roll(t, 127, 1) for t in tiles], axis=1)
        return jnp.concatenate([left, jnp.concatenate(tiles, axis=1), right], axis=0)

    def kgrad(tiles, gref, b):
        rhs = jnp.concatenate([gref[pl.ds(2 * b, 4), j].reshape(256, 128) for j in range(8)], axis=1)
        return lax.dot_general(shifted(tiles), rhs, (((1,), (1,)), ((), ())), preferred_element_type=F32)

    def group_blocks(g):
        return [lax.rem(4 * g + k + n_blocks - 2, n_blocks) for k in range(4)]

    def middle(i, carry):
        @pl.when(i < n_groups - 1)
        def _():
            g_pair(i, theirs).wait_recv()

        bsum = None
        dw = None
        for b in group_blocks(i):
            tiles = [jnp.concatenate([packed(raw_a, 2 * b + r, j) for r in range(2)], axis=0) for j in range(8)]
            for q in range(4):
                for s, o in enumerate(conv_tile(g_all, wm_two, b, q)):
                    j = 2 * q + s
                    m = jnp.where(tiles[j].astype(F32) > 0, o, 0.0)
                    bsum = m if bsum is None else bsum + m
                    z = m.astype(BF16)
                    for r in range(2):
                        z_all[2 * b + 1 + r, j, mine] = z[r * 32:(r + 1) * 32]
            part = kgrad(tiles, g_all, b)
            dw = part if dw is None else dw + part
        bacc[...] += bsum
        acc[...] += dw

        @pl.when(i == 0)
        def _():
            for up in range(2):
                for rel in range(2):
                    halo(z_all, up, rel, zh_send, zh_recv).start()

        for part in range(2):
            z_pair(i, part, mine).start()
        return carry

    g_pair(n_groups - 1, theirs).wait_recv()
    halo_finish(g_all, gh_send, gh_recv)
    load_a.wait()
    lax.fori_loop(0, n_groups, middle, 0)

    def reduce_copy(i, p, t, k, slot):
        axis = (p + t) % 3
        ref = red.at[i, p, t, slot]
        return pltpu.make_async_remote_copy(src_ref=ref, dst_ref=ref, send_sem=ar_send.at[i, p, t, k - 1], recv_sem=ar_recv.at[i, p, t, k - 1],
                                            device_id={"sp": ring_peer(axis, k), "tp": tp}, device_id_type=MESH)

    def reduce_start(i, p):
        for t in range(3):
            for k in range(1, side):
                reduce_copy(i, p, t, k, coords[(p + t) % 3]).start()

    def reduce_begin(i, extra):
        for t in range(3):
            top = acc[pl.ds(t * 64, 32), :]
            low = acc[pl.ds(t * 64 + 32, 32), :]
            e = top[:, 0:192] + low[:, 64:256]
            tail = extra if t == 0 else jnp.zeros((32, 64), F32)
            red[i, 0, t, coords[t]] = jnp.concatenate([e, tail], axis=1)
        reduce_start(i, 0)

    def reduce_step(i, p):
        for t in range(3):
            axis = (p + t) % 3
            me = coords[axis]
            for k in range(1, side):
                reduce_copy(i, p, t, k, lax.rem(me - k + side, side)).wait_recv()
            total = red[i, p, t, 0]
            for c in range(1, side):
                total = total + red[i, p, t, c]
            if p < 2:
                red[i, p + 1, t, coords[(p + 1 + t) % 3]] = total
            else:
                out = (dw_one, dw_two)[i]
                for kh in range(3):
                    out[kh, t] = total[:, (2 - kh) * 64:(3 - kh) * 64]
                if i == 0 and t == 0:
                    wide = jnp.concatenate([total[:, 192:256], jnp.zeros((32, 64), F32)], axis=1)
                    dbias[...] = jnp.sum(wide.T, axis=0, keepdims=True)
        if p < 2:
            reduce_start(i, p + 1)

    reduce_begin(1, jnp.zeros((32, 64), F32))
    acc[...] = jnp.zeros_like(acc)

    def tail_grad(i, carry):
        @pl.when(i < n_groups - 2)
        def _():
            for part in range(2):
                z_pair(i + 2, part, theirs).wait_recv()

        dw = None
        for b in group_blocks(lax.rem(i + 1, n_groups)):
            tiles = [jnp.concatenate([packed(raw_x, 2 * b + r, j) for r in range(2)], axis=0) for j in range(8)]
            part = kgrad(tiles, z_all, b)
            dw = part if dw is None else dw + part
        acc[...] += dw
        return carry

    load_x.wait()
    for g in range(2):
        for part in range(2):
            z_pair(g, part, theirs).wait_recv()
    halo_finish(z_all, zh_send, zh_recv)
    lax.fori_loop(0, n_groups, tail_grad, 0)
    both = bacc[0:32, :] + bacc[32:64, :]
    reduce_begin(0, both[:, 0:64] + both[:, 64:128])
    reduce_step(1, 0)

    def store(c):
        part = pl.ds(c * 8, 8)
        return pltpu.make_async_copy(raw_g.at[:, part], dx_hbm.at[:, part], out_sem.at[c])

    def last(c, carry):
        for k in range(4):
            b = 4 * c + k
            for q in range(4):
                for s, o in enumerate(conv_tile(z_all, wm_one, b, q)):
                    j = 2 * q + s
                    for r in range(2):
                        gy = g_all[2 * b + 1 + r, j, mine].astype(F32)
                        v = (gy + o[r * 32:(r + 1) * 32]).astype(BF16)
                        raw_g[j, 2 * b + r] = v[:, 0:56]
                        raw_g[j + 8, 2 * b + r] = v[:, 64:120]
        store(c).start()
        return carry

    third = max(n_groups // 3, 1)
    lax.fori_loop(0, third, last, 0)
    reduce_step(1, 1)
    reduce_step(0, 0)
    lax.fori_loop(third, min(2 * third, n_groups), last, 0)
    reduce_step(1, 2)
    reduce_step(0, 1)
    lax.fori_loop(min(2 * third, n_groups), n_groups, last, 0)
    reduce_step(0, 2)

    for c in range(n_groups):
        store(c).wait()
        g_pair(c, mine).wait_send()
        for part in range(2):
            z_pair(c, part, mine).wait_send()
    for up in range(2):
        for rel in range(2):
            halo(g_all, up, rel, gh_send, gh_recv).wait_send()
            halo(z_all, up, rel, zh_send, zh_recv).wait_send()
    for i in range(2):
        for p in range(3):
            for t in range(3):
                for k in range(1, side):
                    reduce_copy(i, p, t, k, coords[(p + t) % 3]).wait_send()


def solution(mesh):
    side = round(mesh.shape["sp"] ** (1 / 3))

    def local_step(x_in, act_saved, w_one, w_two, d_out):
        swap = lambda v: jnp.transpose(v, (0, 1, 3, 2))
        imgs, rows, width, ch = x_in.shape
        n_groups = rows // 8
        raw = pltpu.VMEM((imgs, rows, ch, width), BF16)
        full = pltpu.VMEM((rows + 2, 8, 64, 128), BF16)
        dma = pltpu.SemaphoreType.DMA
        vmem = pl.BlockSpec(memory_space=pltpu.VMEM)
        hbm = pl.BlockSpec(memory_space=pl.ANY)
        dx, dw_one, dw_two, dbias = pl.pallas_call(
            functools.partial(body, side, rows),
            out_shape=(
                jax.ShapeDtypeStruct((imgs, rows, ch, width), BF16),
                jax.ShapeDtypeStruct((3, 3, 32, 64), F32),
                jax.ShapeDtypeStruct((3, 3, 32, 64), F32),
                jax.ShapeDtypeStruct((1, 32), F32),
            ),
            in_specs=[hbm, hbm, hbm, vmem, vmem],
            out_specs=(hbm, vmem, vmem, vmem),
            scratch_shapes=[
                raw, raw, raw, full, full,
                pltpu.VMEM((192, 256), BF16), pltpu.VMEM((192, 256), BF16),
                pltpu.VMEM((192, 256), F32), pltpu.VMEM((64, 128), F32),
                pltpu.VMEM((2, 3, 3, side, 32, 256), F32),
                dma((n_groups,)), dma, dma, dma((n_groups,)),
                dma((n_groups,)), dma((n_groups,)), dma((2, 2)), dma((2, 2)),
                dma((n_groups, 2)), dma((n_groups, 2)), dma((2, 2)), dma((2, 2)),
                dma((2, 3, 3, side - 1)), dma((2, 3, 3, side - 1)),
            ],
            compiler_params=pltpu.CompilerParams(collective_id=0, has_side_effects=True, vmem_limit_bytes=60 * 1024 * 1024),
            name="resblock_bwd",
        )(swap(x_in), swap(act_saved), swap(d_out), w_one, w_two)
        return swap(dx), dw_one, dw_two, dbias.reshape(32)

    act_spec = P("dp", "sp", None, "tp")
    kern_spec = P(None, None, "tp", None)
    grad_spec = P("dp", None, "tp", None)
    return jax.shard_map(local_step, mesh=mesh, in_specs=(act_spec, act_spec, kern_spec, kern_spec, act_spec),
                         out_specs=(act_spec, grad_spec, grad_spec, P(("dp", "tp"))), check_vma=False)
```

```python
import functools

import jax
import jax.numpy as jnp
from jax import lax
from jax.experimental import pallas as pl
from jax.experimental.pallas import tpu as pltpu
from jax.sharding import PartitionSpec as P

MESH = pl.DeviceIdType.MESH
BF16 = jnp.bfloat16
F32 = jnp.float32


def body(side, rows, x_hbm, a_hbm, g_hbm, w_one, w_two, dx_hbm, dw_one, dw_two, dbias,
         raw_g, raw_a, raw_x, g_all, z_all, wm_one, wm_two, acc, bacc, red,
         g_sem, a_sem, x_sem, out_sem, gx_send, gx_recv, gh_send, gh_recv, zx_send, zx_recv, zh_send, zh_recv,
         ar_send, ar_recv):
    sp = lax.axis_index("sp")
    tp = lax.axis_index("tp")
    row_devs = side * side * side
    n_groups = rows // 8
    n_blocks = rows // 2
    coords = (lax.rem(sp, side), lax.rem(lax.div(sp, side), side), lax.div(sp, side * side))
    strides = (1, side, side * side)
    nxt = lax.rem(sp + 1, row_devs)
    prv = lax.rem(sp + row_devs - 1, row_devs)
    other = 1 - tp
    mine = pl.ds(pl.multiple_of(tp * 32, 32), 32)
    theirs = pl.ds(pl.multiple_of(other * 32, 32), 32)

    def ring_peer(axis, k):
        me = coords[axis]
        return sp + (lax.rem(me + k, side) - me) * strides[axis]

    def load_g(c):
        part = pl.ds(c * 8, 8)
        return pltpu.make_async_copy(g_hbm.at[:, part], raw_g.at[:, part], g_sem.at[c])

    load_a = pltpu.make_async_copy(a_hbm, raw_a, a_sem)
    load_x = pltpu.make_async_copy(x_hbm, raw_x, x_sem)

    for i in range(n_groups):
        load_g((i + n_groups - 1) % n_groups).start()

    barrier = pltpu.get_barrier_semaphore()
    targets = [(sp, other), (nxt, tp), (nxt, other), (prv, tp), (prv, other)]
    for axis in range(3):
        for k in range(1, side):
            targets.append((ring_peer(axis, k), tp))
    for s, t in targets:
        pl.semaphore_signal(barrier, inc=1, device_id={"sp": s, "tp": t}, device_id_type=MESH)
    load_a.start()

    for w_ref, wm in ((w_two, wm_two), (w_one, wm_one)):
        for kw in range(3):
            for r in range(2):
                blocks = []
                for rr in range(4):
                    kh = r + 2 - rr
                    blocks.append(w_ref[kh, kw] if 0 <= kh < 3 else jnp.zeros((32, 64), BF16))
                wm[pl.ds(kw * 64 + r * 32, 32), :] = jnp.concatenate(blocks, axis=1)
    bacc[...] = jnp.zeros_like(bacc)
    acc[...] = jnp.zeros_like(acc)

    def packed(raw, h, j):
        gap = jnp.zeros((32, 8), BF16)
        return jnp.concatenate([raw[j, h], gap, raw[j + 8, h], gap], axis=1)

    def remote(ref, lo, n, sl, send, recv):
        part = ref.at[pl.ds(lo, n), :, sl]
        return pltpu.make_async_remote_copy(src_ref=part, dst_ref=part, send_sem=send, recv_sem=recv,
                                            device_id={"sp": sp, "tp": other}, device_id_type=MESH)

    def halo(ref, up, rel, send, recv):
        src_row, dst_row, dev = (rows, 0, nxt) if up == 0 else (1, rows + 1, prv)
        return pltpu.make_async_remote_copy(
            src_ref=ref.at[src_row, :, mine], dst_ref=ref.at[dst_row, :, mine], send_sem=send.at[up, rel], recv_sem=recv.at[up, rel],
            device_id={"sp": dev, "tp": tp if rel == 0 else other}, device_id_type=MESH)

    def halo_finish(ref, send, recv):
        for up in range(2):
            for rel in range(2):
                dst_row, dev = (0, prv) if up == 0 else (rows + 1, nxt)
                part = ref.at[dst_row, :, mine if rel == 0 else theirs]
                pltpu.make_async_remote_copy(
                    src_ref=part, dst_ref=part, send_sem=send.at[up, rel], recv_sem=recv.at[up, rel],
                    device_id={"sp": dev, "tp": tp if rel == 0 else other}, device_id_type=MESH).wait_recv()

        @pl.when(sp == 0)
        def _():
            ref[0] = jnp.zeros((8, 64, 128), BF16)

        @pl.when(sp == row_devs - 1)
        def _():
            ref[rows + 1] = jnp.zeros((8, 64, 128), BF16)

    def g_pair(c, sl):
        return remote(g_all, c * 8 + 1, 8, sl, gx_send.at[c], gx_recv.at[c])

    def z_pair(g, part, sl):
        lo = lax.rem(8 * g + part * 4 + rows - 4, rows) + 1
        return remote(z_all, lo, 4, sl, zx_send.at[g, part], zx_recv.at[g, part])

    pl.semaphore_wait(barrier, len(targets))

    def pack_g(i, carry):
        c = lax.rem(i + n_groups - 1, n_groups)
        load_g(c).wait()
        for h in range(8):
            for j in range(8):
                g_all[c * 8 + h + 1, j, mine] = packed(raw_g, c * 8 + h, j)

        @pl.when(i == 0)
        def _():
            for rel in range(2):
                halo(g_all, 0, rel, gh_send, gh_recv).start()

        @pl.when(i == 1)
        def _():
            for rel in range(2):
                halo(g_all, 1, rel, gh_send, gh_recv).start()

        g_pair(c, mine).start()
        return carry

    lax.fori_loop(0, n_groups, pack_g, 0)
    load_x.start()

    def conv_tile(src, wm, b, q):
        tile = jnp.concatenate([src[pl.ds(2 * b, 4), 2 * q + s].reshape(256, 128) for s in range(2)], axis=1)
        d = jnp.dot(wm[...], tile, preferred_element_type=F32)
        outs = []
        for s in range(2):
            part = d[:, s * 128:(s + 1) * 128]
            outs.append(part[64:128] + pltpu.roll(part[0:64], 127, 1) + pltpu.roll(part[128:192], 1, 1))
        return outs

    def shifted(tiles):
        left = jnp.concatenate([pltpu.roll(t, 1, 1) for t in tiles], axis=1)
        right = jnp.concatenate([pltpu.roll(t, 127, 1) for t in tiles], axis=1)
        return jnp.concatenate([left, jnp.concatenate(tiles, axis=1), right], axis=0)

    def kgrad(tiles, gref, b):
        rhs = jnp.concatenate([gref[pl.ds(2 * b, 4), j].reshape(256, 128) for j in range(8)], axis=1)
        return lax.dot_general(shifted(tiles), rhs, (((1,), (1,)), ((), ())), preferred_element_type=F32)

    def group_blocks(g):
        return [lax.rem(4 * g + k + n_blocks - 2, n_blocks) for k in range(4)]

    def middle(i, carry):
        @pl.when(i < n_groups - 1)
        def _():
            g_pair(i, theirs).wait_recv()

        bsum = None
        dw = None
        for b in group_blocks(i):
            tiles = [jnp.concatenate([packed(raw_a, 2 * b + r, j) for r in range(2)], axis=0) for j in range(8)]
            for q in range(4):
                for s, o in enumerate(conv_tile(g_all, wm_two, b, q)):
                    j = 2 * q + s
                    m = jnp.where(tiles[j].astype(F32) > 0, o, 0.0)
                    bsum = m if bsum is None else bsum + m
                    z = m.astype(BF16)
                    for r in range(2):
                        z_all[2 * b + 1 + r, j, mine] = z[r * 32:(r + 1) * 32]
            part = kgrad(tiles, g_all, b)
            dw = part if dw is None else dw + part
        bacc[...] += bsum
        acc[...] += dw

        @pl.when(i == 0)
        def _():
            for up in range(2):
                for rel in range(2):
                    halo(z_all, up, rel, zh_send, zh_recv).start()

        for part in range(2):
            z_pair(i, part, mine).start()
        return carry

    g_pair(n_groups - 1, theirs).wait_recv()
    halo_finish(g_all, gh_send, gh_recv)
    load_a.wait()
    lax.fori_loop(0, n_groups, middle, 0)

    def reduce_copy(i, p, t, k, slot):
        axis = (p + t) % 3
        ref = red.at[i, p, t, slot]
        return pltpu.make_async_remote_copy(src_ref=ref, dst_ref=ref, send_sem=ar_send.at[i, p, t, k - 1], recv_sem=ar_recv.at[i, p, t, k - 1],
                                            device_id={"sp": ring_peer(axis, k), "tp": tp}, device_id_type=MESH)

    def reduce_start(i, p):
        for t in range(3):
            for k in range(1, side):
                reduce_copy(i, p, t, k, coords[(p + t) % 3]).start()

    def reduce_begin(i, extra):
        for t in range(3):
            top = acc[pl.ds(t * 64, 32), :]
            low = acc[pl.ds(t * 64 + 32, 32), :]
            e = top[:, 0:192] + low[:, 64:256]
            tail = extra if t == 0 else jnp.zeros((32, 64), F32)
            red[i, 0, t, coords[t]] = jnp.concatenate([e, tail], axis=1)
        reduce_start(i, 0)

    def reduce_step(i, p):
        for t in range(3):
            axis = (p + t) % 3
            me = coords[axis]
            for k in range(1, side):
                reduce_copy(i, p, t, k, lax.rem(me - k + side, side)).wait_recv()
            total = red[i, p, t, 0]
            for c in range(1, side):
                total = total + red[i, p, t, c]
            if p < 2:
                red[i, p + 1, t, coords[(p + 1 + t) % 3]] = total
            else:
                out = (dw_one, dw_two)[i]
                for kh in range(3):
                    out[kh, t] = total[:, (2 - kh) * 64:(3 - kh) * 64]
                if i == 0 and t == 0:
                    wide = jnp.concatenate([total[:, 192:256], jnp.zeros((32, 64), F32)], axis=1)
                    dbias[...] = jnp.sum(wide.T, axis=0, keepdims=True)
        if p < 2:
            reduce_start(i, p + 1)

    reduce_begin(1, jnp.zeros((32, 64), F32))
    acc[...] = jnp.zeros_like(acc)

    def tail_grad(i, carry):
        @pl.when(i < n_groups - 2)
        def _():
            for part in range(2):
                z_pair(i + 2, part, theirs).wait_recv()

        dw = None
        for b in group_blocks(lax.rem(i + 1, n_groups)):
            tiles = [jnp.concatenate([packed(raw_x, 2 * b + r, j) for r in range(2)], axis=0) for j in range(8)]
            part = kgrad(tiles, z_all, b)
            dw = part if dw is None else dw + part
        acc[...] += dw
        return carry

    load_x.wait()
    for g in range(2):
        for part in range(2):
            z_pair(g, part, theirs).wait_recv()
    halo_finish(z_all, zh_send, zh_recv)
    lax.fori_loop(0, n_groups, tail_grad, 0)
    both = bacc[0:32, :] + bacc[32:64, :]
    reduce_begin(0, both[:, 0:64] + both[:, 64:128])
    reduce_step(1, 0)

    def last(c, carry):
        for k in range(4):
            b = 4 * c + k
            for q in range(4):
                for s, o in enumerate(conv_tile(z_all, wm_one, b, q)):
                    j = 2 * q + s
                    for r in range(2):
                        gy = g_all[2 * b + 1 + r, j, mine].astype(F32)
                        v = (gy + o[r * 32:(r + 1) * 32]).astype(BF16)
                        dx_hbm[j, 2 * b + r] = v[:, 0:56]
                        dx_hbm[j + 8, 2 * b + r] = v[:, 64:120]
        return carry

    third = max(n_groups // 3, 1)
    lax.fori_loop(0, third, last, 0)
    reduce_step(1, 1)
    reduce_step(0, 0)
    lax.fori_loop(third, min(2 * third, n_groups), last, 0)
    reduce_step(1, 2)
    reduce_step(0, 1)
    lax.fori_loop(min(2 * third, n_groups), n_groups, last, 0)
    reduce_step(0, 2)

    for c in range(n_groups):
        g_pair(c, mine).wait_send()
        for part in range(2):
            z_pair(c, part, mine).wait_send()
    for up in range(2):
        for rel in range(2):
            halo(g_all, up, rel, gh_send, gh_recv).wait_send()
            halo(z_all, up, rel, zh_send, zh_recv).wait_send()
    for i in range(2):
        for p in range(3):
            for t in range(3):
                for k in range(1, side):
                    reduce_copy(i, p, t, k, coords[(p + t) % 3]).wait_send()


def solution(mesh):
    side = round(mesh.shape["sp"] ** (1 / 3))

    def local_step(x_in, act_saved, w_one, w_two, d_out):
        swap = lambda v: jnp.transpose(v, (0, 1, 3, 2))
        imgs, rows, width, ch = x_in.shape
        n_groups = rows // 8
        raw = pltpu.VMEM((imgs, rows, ch, width), BF16)
        full = pltpu.VMEM((rows + 2, 8, 64, 128), BF16)
        dma = pltpu.SemaphoreType.DMA
        vmem = pl.BlockSpec(memory_space=pltpu.VMEM)
        hbm = pl.BlockSpec(memory_space=pl.ANY)
        dx, dw_one, dw_two, dbias = pl.pallas_call(
            functools.partial(body, side, rows),
            out_shape=(
                pltpu.VMEM((imgs, rows, ch, width), BF16),
                pltpu.VMEM((3, 3, 32, 64), F32),
                pltpu.VMEM((3, 3, 32, 64), F32),
                pltpu.VMEM((1, 32), F32),
            ),
            in_specs=[hbm, hbm, hbm, vmem, vmem],
            out_specs=(vmem, vmem, vmem, vmem),
            scratch_shapes=[
                raw, raw, raw, full, full,
                pltpu.VMEM((192, 256), BF16), pltpu.VMEM((192, 256), BF16),
                pltpu.VMEM((192, 256), F32), pltpu.VMEM((64, 128), F32),
                pltpu.VMEM((2, 3, 3, side, 32, 256), F32),
                dma((n_groups,)), dma, dma, dma((n_groups,)),
                dma((n_groups,)), dma((n_groups,)), dma((2, 2)), dma((2, 2)),
                dma((n_groups, 2)), dma((n_groups, 2)), dma((2, 2)), dma((2, 2)),
                dma((2, 3, 3, side - 1)), dma((2, 3, 3, side - 1)),
            ],
            compiler_params=pltpu.CompilerParams(collective_id=0, has_side_effects=True, vmem_limit_bytes=46 * 1024 * 1024),
            name="resblock_bwd",
        )(swap(x_in), swap(act_saved), swap(d_out), w_one, w_two)
        return swap(dx), dw_one, dw_two, dbias.reshape(32)

    act_spec = P("dp", "sp", None, "tp")
    kern_spec = P(None, None, "tp", None)
    grad_spec = P("dp", None, "tp", None)
    return jax.shard_map(local_step, mesh=mesh, in_specs=(act_spec, act_spec, kern_spec, kern_spec, act_spec),
                         out_specs=(act_spec, grad_spec, grad_spec, P(("dp", "tp"))), check_vma=False)
```

```python
import functools

import jax
import jax.numpy as jnp
from jax import lax
from jax.experimental import pallas as pl
from jax.experimental.pallas import tpu as pltpu
from jax.sharding import PartitionSpec as P

MESH = pl.DeviceIdType.MESH
BF16 = jnp.bfloat16
F32 = jnp.float32


def body(side, rows, x_hbm, a_hbm, g_hbm, w_one, w_two, dx_hbm, dw_one, dw_two, dbias,
         raw_g, raw_a, raw_x, g_all, z_all, w_raw, wm_one, wm_two, acc, bacc, red,
         g_sem, a_sem, x_sem, w_sem, gx_send, gx_recv, gh_send, gh_recv, zx_send, zx_recv, zh_send, zh_recv,
         ar_send, ar_recv):
    sp = lax.axis_index("sp")
    tp = lax.axis_index("tp")
    row_devs = side * side * side
    n_groups = rows // 8
    n_blocks = rows // 2
    coords = (lax.rem(sp, side), lax.rem(lax.div(sp, side), side), lax.div(sp, side * side))
    strides = (1, side, side * side)
    nxt = lax.rem(sp + 1, row_devs)
    prv = lax.rem(sp + row_devs - 1, row_devs)
    other = 1 - tp
    mine = pl.ds(pl.multiple_of(tp * 32, 32), 32)
    theirs = pl.ds(pl.multiple_of(other * 32, 32), 32)

    def ring_peer(axis, k):
        me = coords[axis]
        return sp + (lax.rem(me + k, side) - me) * strides[axis]

    def load(hbm, raw, sem, c):
        part = pl.ds(c * 8, 8)
        return pltpu.make_async_copy(hbm.at[:, part], raw.at[:, part], sem.at[c])

    def load_g(c):
        return load(g_hbm, raw_g, g_sem, c)

    def load_a(c):
        return load(a_hbm, raw_a, a_sem, c)

    load_x = pltpu.make_async_copy(x_hbm, raw_x, x_sem)
    load_w = [pltpu.make_async_copy(w, w_raw.at[i], w_sem.at[i]) for i, w in enumerate((w_one, w_two))]

    load_g(0).start()
    for w in load_w:
        w.start()
    for c in range(1, min(3, n_groups)):
        load_g(c).start()
    load_a(0).start()

    barrier = pltpu.get_barrier_semaphore()
    targets = [(sp, other), (nxt, tp), (nxt, other), (prv, tp), (prv, other)]
    for axis in range(3):
        for k in range(1, side):
            targets.append((ring_peer(axis, k), tp))
    for s, t in targets:
        pl.semaphore_signal(barrier, inc=1, device_id={"sp": s, "tp": t}, device_id_type=MESH)

    for i, wm in ((1, wm_two), (0, wm_one)):
        load_w[i].wait()
        for kw in range(3):
            for r in range(2):
                blocks = []
                for rr in range(4):
                    kh = r + 2 - rr
                    blocks.append(w_raw[i, kh, kw] if 0 <= kh < 3 else jnp.zeros((32, 64), BF16))
                wm[pl.ds(kw * 64 + r * 32, 32), :] = jnp.concatenate(blocks, axis=1)
    bacc[...] = jnp.zeros_like(bacc)
    acc[...] = jnp.zeros_like(acc)

    def packed(raw, h, j):
        gap = jnp.zeros((32, 8), BF16)
        return jnp.concatenate([raw[j, h], gap, raw[j + 8, h], gap], axis=1)

    def remote(ref, lo, n, sl, send, recv):
        part = ref.at[pl.ds(lo, n), :, sl]
        return pltpu.make_async_remote_copy(src_ref=part, dst_ref=part, send_sem=send, recv_sem=recv,
                                            device_id={"sp": sp, "tp": other}, device_id_type=MESH)

    def halo(ref, up, rel, send, recv):
        src_row, dst_row, dev = (rows, 0, nxt) if up == 0 else (1, rows + 1, prv)
        return pltpu.make_async_remote_copy(
            src_ref=ref.at[src_row, :, mine], dst_ref=ref.at[dst_row, :, mine], send_sem=send.at[up, rel], recv_sem=recv.at[up, rel],
            device_id={"sp": dev, "tp": tp if rel == 0 else other}, device_id_type=MESH)

    def halo_finish(ref, send, recv):
        for up in range(2):
            for rel in range(2):
                dst_row, dev = (0, prv) if up == 0 else (rows + 1, nxt)
                part = ref.at[dst_row, :, mine if rel == 0 else theirs]
                pltpu.make_async_remote_copy(
                    src_ref=part, dst_ref=part, send_sem=send.at[up, rel], recv_sem=recv.at[up, rel],
                    device_id={"sp": dev, "tp": tp if rel == 0 else other}, device_id_type=MESH).wait_recv()

        @pl.when(sp == 0)
        def _():
            ref[0] = jnp.zeros((8, 64, 128), BF16)

        @pl.when(sp == row_devs - 1)
        def _():
            ref[rows + 1] = jnp.zeros((8, 64, 128), BF16)

    def g_pair(c, sl):
        return remote(g_all, c * 8 + 1, 8, sl, gx_send.at[c], gx_recv.at[c])

    def z_pair(g, part, sl):
        lo = lax.rem(8 * g + part * 4 + rows - 4, rows) + 1
        return remote(z_all, lo, 4, sl, zx_send.at[g, part], zx_recv.at[g, part])

    pl.semaphore_wait(barrier, len(targets))

    def pack_rows(c):
        for h in range(8):
            for j in range(8):
                g_all[c * 8 + h + 1, j, mine] = packed(raw_g, c * 8 + h, j)

    def pack_g(c, carry):
        load_g(c).wait()
        pack_rows(c)

        @pl.when(c == 0)
        def _():
            for rel in range(2):
                halo(g_all, 1, rel, gh_send, gh_recv).start()

        g_pair(c, mine).start()

        @pl.when(c + ahead < n_groups)
        def _():
            load_g(c + ahead).start()

        load_a(c + 1).start()
        return carry

    ahead = min(3, n_groups - 1)
    lax.fori_loop(0, ahead, pack_g, 0)
    for c in range(ahead + 1, n_groups):
        load_a(c).start()
    load_x.start()

    def conv_tile(src, wm, b, q):
        tile = jnp.concatenate([src[pl.ds(2 * b, 4), 2 * q + s].reshape(256, 128) for s in range(2)], axis=1)
        d = jnp.dot(wm[...], tile, preferred_element_type=F32)
        outs = []
        for s in range(2):
            part = d[:, s * 128:(s + 1) * 128]
            outs.append(part[64:128] + pltpu.roll(part[0:64], 127, 1) + pltpu.roll(part[128:192], 1, 1))
        return outs

    def shifted(tiles):
        left = jnp.concatenate([pltpu.roll(t, 1, 1) for t in tiles], axis=1)
        right = jnp.concatenate([pltpu.roll(t, 127, 1) for t in tiles], axis=1)
        return jnp.concatenate([left, jnp.concatenate(tiles, axis=1), right], axis=0)

    def kgrad(tiles, gref, b):
        rhs = jnp.concatenate([gref[pl.ds(2 * b, 4), j].reshape(256, 128) for j in range(8)], axis=1)
        return lax.dot_general(shifted(tiles), rhs, (((1,), (1,)), ((), ())), preferred_element_type=F32)

    def group_blocks(g):
        return [lax.rem(4 * g + k + n_blocks - 2, n_blocks) for k in range(4)]

    def middle(i, ahead):
        if ahead:
            load_g(i + ahead).wait()

        @pl.when(i + 1 < n_groups)
        def _():
            load_a(i + 1).wait()
            g_pair(i + 1, theirs).wait_recv()

        if ahead:
            pack_rows(i + ahead)
        g = lax.rem(i + 1, n_groups)
        bsum = None
        dw = None
        for b in group_blocks(g):
            tiles = [jnp.concatenate([packed(raw_a, 2 * b + r, j) for r in range(2)], axis=0) for j in range(8)]
            for q in range(4):
                for s, o in enumerate(conv_tile(g_all, wm_two, b, q)):
                    j = 2 * q + s
                    m = jnp.where(tiles[j].astype(F32) > 0, o, 0.0)
                    bsum = m if bsum is None else bsum + m
                    z = m.astype(BF16)
                    for r in range(2):
                        z_all[2 * b + 1 + r, j, mine] = z[r * 32:(r + 1) * 32]
            part = kgrad(tiles, g_all, b)
            dw = part if dw is None else dw + part
        bacc[...] += bsum
        acc[...] += dw
        if ahead:
            g_pair(i + ahead, mine).start()

            @pl.when(i + ahead == n_groups - 1)
            def _():
                for rel in range(2):
                    halo(g_all, 0, rel, gh_send, gh_recv).start()

        for part in range(2):
            z_pair(g, part, mine).start()

    load_a(0).wait()
    g_pair(0, theirs).wait_recv()

    def middle_pack(i, carry):
        middle(i, ahead)
        return carry

    def middle_plain(i, carry):
        @pl.when(i == n_groups - 1)
        def _():
            halo_finish(g_all, gh_send, gh_recv)

        middle(i, 0)
        return carry

    lax.fori_loop(0, n_groups - ahead, middle_pack, 0)
    lax.fori_loop(n_groups - ahead, n_groups, middle_plain, 0)
    for up in range(2):
        for rel in range(2):
            halo(z_all, up, rel, zh_send, zh_recv).start()

    def reduce_copy(i, p, t, k, slot):
        axis = (p + t) % 3
        ref = red.at[i, p, t, slot, pl.ds(0, 56 if i == 0 and t == 0 else 48)]
        return pltpu.make_async_remote_copy(src_ref=ref, dst_ref=ref, send_sem=ar_send.at[i, p, t, k - 1], recv_sem=ar_recv.at[i, p, t, k - 1],
                                            device_id={"sp": ring_peer(axis, k), "tp": tp}, device_id_type=MESH)

    def reduce_start(i, p):
        for t in range(3):
            for k in (2, 1, 3)[:side - 1] if side > 2 else (1,):
                reduce_copy(i, p, t, k, coords[(p + t) % 3]).start()

    def reduce_begin(i):
        for t in range(3):
            top = acc[pl.ds(t * 64, 32), :]
            low = acc[pl.ds(t * 64 + 32, 32), :]
            e = top[:, 0:192] + low[:, 64:256]
            red[i, 0, t, coords[t], pl.ds(0, 32)] = e[:, 0:128]
            red[i, 0, t, coords[t], pl.ds(32, 16)] = jnp.concatenate([e[0:16, 128:192], e[16:32, 128:192]], axis=1)
            if i == 0 and t == 0:
                both = bacc[0:32, :] + bacc[32:64, :]
                col = jnp.sum(both, axis=1, keepdims=True)
                row = jnp.broadcast_to(col, (32, 128)).T[0:8]
                red[i, 0, t, coords[t], pl.ds(48, 8)] = jnp.concatenate([row, jnp.zeros((8, 96), F32)], axis=1)
        reduce_start(i, 0)

    def reduce_step(i, p):
        for t in range(3):
            n = 56 if i == 0 and t == 0 else 48
            axis = (p + t) % 3
            me = coords[axis]
            for k in range(1, side):
                reduce_copy(i, p, t, k, lax.rem(me - k + side, side)).wait_recv()
            total = red[i, p, t, 0, pl.ds(0, n)]
            for c in range(1, side):
                total = total + red[i, p, t, c, pl.ds(0, n)]
            if p < 2:
                red[i, p + 1, t, coords[(p + 1 + t) % 3], pl.ds(0, n)] = total
            else:
                out = (dw_one, dw_two)[i]
                out[2, t] = total[0:32, 0:64]
                out[1, t] = total[0:32, 64:128]
                out[0, t] = jnp.concatenate([total[32:48, 0:64], total[32:48, 64:128]], axis=0)
                if i == 0 and t == 0:
                    dbias[...] = total[48:49, 0:32]
        if p < 2:
            reduce_start(i, p + 1)

    reduce_begin(1)
    acc[...] = jnp.zeros_like(acc)

    def z_wait(g):
        for part in range(2):
            z_pair(g, part, theirs).wait_recv()

    def tail_grad(i, carry):
        @pl.when((i > 0) & (i < n_groups - 2))
        def _():
            z_wait(lax.rem(i + 3, n_groups))

        @pl.when(i == n_groups - 2)
        def _():
            halo_finish(z_all, zh_send, zh_recv)

        dw = None
        for b in group_blocks(lax.rem(i + 2, n_groups)):
            tiles = [jnp.concatenate([packed(raw_x, 2 * b + r, j) for r in range(2)], axis=0) for j in range(8)]
            part = kgrad(tiles, z_all, b)
            dw = part if dw is None else dw + part
        acc[...] += dw
        return carry

    load_x.wait()
    for g in range(1, min(4, n_groups)):
        z_wait(g)
    lax.fori_loop(0, n_groups - 2, tail_grad, 0)
    reduce_step(1, 0)
    lax.fori_loop(n_groups - 2, n_groups, tail_grad, 0)
    reduce_begin(0)

    def last(c, carry):
        for k in range(4):
            b = 4 * c + k
            for q in range(4):
                for s, o in enumerate(conv_tile(z_all, wm_one, b, q)):
                    j = 2 * q + s
                    for r in range(2):
                        gy = g_all[2 * b + 1 + r, j, mine].astype(F32)
                        v = (gy + o[r * 32:(r + 1) * 32]).astype(BF16)
                        dx_hbm[j, 2 * b + r] = v[:, 0:56]
                        dx_hbm[j + 8, 2 * b + r] = v[:, 64:120]
        return carry

    third = max(n_groups // 3, 1)
    lax.fori_loop(0, third, last, 0)
    reduce_step(1, 1)
    reduce_step(0, 0)
    lax.fori_loop(third, min(2 * third, n_groups), last, 0)
    reduce_step(1, 2)
    reduce_step(0, 1)
    lax.fori_loop(min(2 * third, n_groups), n_groups, last, 0)
    reduce_step(0, 2)

    for c in range(n_groups):
        g_pair(c, mine).wait_send()
        for part in range(2):
            z_pair(c, part, mine).wait_send()
    for up in range(2):
        for rel in range(2):
            halo(g_all, up, rel, gh_send, gh_recv).wait_send()
            halo(z_all, up, rel, zh_send, zh_recv).wait_send()
    for i in range(2):
        for p in range(3):
            for t in range(3):
                for k in range(1, side):
                    reduce_copy(i, p, t, k, coords[(p + t) % 3]).wait_send()


def write_out(*refs):
    sems = refs[8]
    copies = [pltpu.make_async_copy(refs[i], refs[4 + i], sems.at[i]) for i in range(4)]
    for copy in copies:
        copy.start()
    for copy in copies:
        copy.wait()


def solution(mesh):
    side = round(mesh.shape["sp"] ** (1 / 3))

    def local_step(x_in, act_saved, w_one, w_two, d_out):
        swap = lambda v: jnp.transpose(v, (0, 1, 3, 2))
        imgs, rows, width, ch = x_in.shape
        n_groups = rows // 8
        raw = pltpu.VMEM((imgs, rows, ch, width), BF16)
        full = pltpu.VMEM((rows + 2, 8, 64, 128), BF16)
        dma = pltpu.SemaphoreType.DMA
        vmem = pl.BlockSpec(memory_space=pltpu.VMEM)
        hbm = pl.BlockSpec(memory_space=pltpu.HBM)
        dx, dw_one, dw_two, dbias = pl.pallas_call(
            functools.partial(body, side, rows),
            out_shape=(
                pltpu.VMEM((imgs, rows, ch, width), BF16),
                pltpu.VMEM((3, 3, 32, 64), F32),
                pltpu.VMEM((3, 3, 32, 64), F32),
                pltpu.VMEM((1, 32), F32),
            ),
            in_specs=[hbm, hbm, hbm, hbm, hbm],
            out_specs=(vmem, vmem, vmem, vmem),
            scratch_shapes=[
                raw, raw, raw, full, full, pltpu.VMEM((2, 3, 3, 32, 64), BF16),
                pltpu.VMEM((192, 256), BF16), pltpu.VMEM((192, 256), BF16),
                pltpu.VMEM((192, 256), F32), pltpu.VMEM((64, 128), F32),
                pltpu.VMEM((2, 3, 3, side, 56, 128), F32),
                dma((n_groups,)), dma((n_groups,)), dma, dma((2,)),
                dma((n_groups,)), dma((n_groups,)), dma((2, 2)), dma((2, 2)),
                dma((n_groups, 2)), dma((n_groups, 2)), dma((2, 2)), dma((2, 2)),
                dma((2, 3, 3, side - 1)), dma((2, 3, 3, side - 1)),
            ],
            compiler_params=pltpu.CompilerParams(collective_id=0, has_side_effects=True, vmem_limit_bytes=46 * 1024 * 1024),
            name="resblock_bwd",
        )(*(pltpu.with_memory_space_constraint(v, pltpu.HBM) for v in (swap(x_in), swap(act_saved), swap(d_out), w_one, w_two)))
        results = (dx, dw_one, dw_two, dbias)
        dx, dw_one, dw_two, dbias = pl.pallas_call(
            write_out,
            out_shape=tuple(jax.ShapeDtypeStruct(v.shape, v.dtype) for v in results),
            in_specs=[vmem] * 4,
            out_specs=(hbm,) * 4,
            scratch_shapes=[dma((4,))],
            compiler_params=pltpu.CompilerParams(vmem_limit_bytes=1024 * 1024),
            name="write_out",
        )(*results)
        return swap(dx), dw_one, dw_two, dbias.reshape(32)

    act_spec = P("dp", "sp", None, "tp")
    kern_spec = P(None, None, "tp", None)
    grad_spec = P("dp", None, "tp", None)
    return jax.shard_map(local_step, mesh=mesh, in_specs=(act_spec, act_spec, kern_spec, kern_spec, act_spec),
                         out_specs=(act_spec, grad_spec, grad_spec, P(("dp", "tp"))), check_vma=False)
```

```python
import functools

import jax
import jax.numpy as jnp
from jax import lax
from jax.experimental import pallas as pl
from jax.experimental.pallas import tpu as pltpu
from jax.sharding import PartitionSpec as P

MESH = pl.DeviceIdType.MESH
BF16 = jnp.bfloat16
F32 = jnp.float32


def body(side, rows, x_hbm, a_hbm, g_hbm, w_one, w_two, dx_hbm, dw_one, dw_two, dbias,
         raw_g, raw_a, raw_x, g_all, z_all, w_raw, wm_one, wm_two, acc, bacc, red,
         g_sem, a_sem, x_sem, w_sem, gx_send, gx_recv, gh_send, gh_recv, zx_send, zx_recv, zh_send, zh_recv,
         ar_send, ar_recv):
    sp = lax.axis_index("sp")
    tp = lax.axis_index("tp")
    row_devs = side * side * side
    n_groups = rows // 8
    n_blocks = rows // 2
    coords = (lax.rem(sp, side), lax.rem(lax.div(sp, side), side), lax.div(sp, side * side))
    strides = (1, side, side * side)
    nxt = lax.rem(sp + 1, row_devs)
    prv = lax.rem(sp + row_devs - 1, row_devs)
    other = 1 - tp
    mine = pl.ds(pl.multiple_of(tp * 32, 32), 32)
    theirs = pl.ds(pl.multiple_of(other * 32, 32), 32)

    def ring_peer(axis, k):
        me = coords[axis]
        return sp + (lax.rem(me + k, side) - me) * strides[axis]

    def load(hbm, raw, sem, c):
        part = pl.ds(c * 8, 8)
        return pltpu.make_async_copy(hbm.at[:, part], raw.at[:, part], sem.at[c])

    def load_g(c):
        return load(g_hbm, raw_g, g_sem, c)

    def load_a(c):
        return load(a_hbm, raw_a, a_sem, c)

    load_x = pltpu.make_async_copy(x_hbm, raw_x, x_sem)
    load_w = [pltpu.make_async_copy(w, w_raw.at[i], w_sem.at[i]) for i, w in enumerate((w_one, w_two))]

    load_g(0).start()
    for w in load_w:
        w.start()
    for c in range(1, min(3, n_groups)):
        load_g(c).start()
    load_a(0).start()

    barrier = pltpu.get_barrier_semaphore()
    targets = [(sp, other), (nxt, tp), (nxt, other), (prv, tp), (prv, other)]
    for axis in range(3):
        for k in range(1, side):
            targets.append((ring_peer(axis, k), tp))
    for s, t in targets:
        pl.semaphore_signal(barrier, inc=1, device_id={"sp": s, "tp": t}, device_id_type=MESH)

    bacc[...] = jnp.zeros_like(bacc)
    acc[...] = jnp.zeros_like(acc)

    def packed(raw, h, j):
        gap = jnp.zeros((32, 8), BF16)
        return jnp.concatenate([raw[j, h], gap, raw[j + 8, h], gap], axis=1)

    def remote(ref, lo, n, sl, send, recv):
        part = ref.at[pl.ds(lo, n), :, sl]
        return pltpu.make_async_remote_copy(src_ref=part, dst_ref=part, send_sem=send, recv_sem=recv,
                                            device_id={"sp": sp, "tp": other}, device_id_type=MESH)

    def halo(ref, up, rel, send, recv):
        src_row, dst_row, dev = (rows, 0, nxt) if up == 0 else (1, rows + 1, prv)
        return pltpu.make_async_remote_copy(
            src_ref=ref.at[src_row, :, mine], dst_ref=ref.at[dst_row, :, mine], send_sem=send.at[up, rel], recv_sem=recv.at[up, rel],
            device_id={"sp": dev, "tp": tp if rel == 0 else other}, device_id_type=MESH)

    def halo_finish(ref, send, recv):
        for up in range(2):
            for rel in range(2):
                dst_row, dev = (0, prv) if up == 0 else (rows + 1, nxt)
                part = ref.at[dst_row, :, mine if rel == 0 else theirs]
                pltpu.make_async_remote_copy(
                    src_ref=part, dst_ref=part, send_sem=send.at[up, rel], recv_sem=recv.at[up, rel],
                    device_id={"sp": dev, "tp": tp if rel == 0 else other}, device_id_type=MESH).wait_recv()

        @pl.when(sp == 0)
        def _():
            ref[0] = jnp.zeros((8, 64, 128), BF16)

        @pl.when(sp == row_devs - 1)
        def _():
            ref[rows + 1] = jnp.zeros((8, 64, 128), BF16)

    def g_pair(c, sl):
        return remote(g_all, c * 8 + 1, 8, sl, gx_send.at[c], gx_recv.at[c])

    def z_pair(g, part, sl):
        lo = lax.rem(8 * g + part * 4 + rows - 4, rows) + 1
        return remote(z_all, lo, 4, sl, zx_send.at[g, part], zx_recv.at[g, part])

    pl.semaphore_wait(barrier, len(targets))

    def pack_rows(c):
        for h in range(8):
            for j in range(8):
                g_all[c * 8 + h + 1, j, mine] = packed(raw_g, c * 8 + h, j)

    def pack_g(c, carry):
        load_g(c).wait()
        pack_rows(c)

        @pl.when(c == 0)
        def _():
            for rel in range(2):
                halo(g_all, 1, rel, gh_send, gh_recv).start()

        g_pair(c, mine).start()

        @pl.when(c + ahead < n_groups)
        def _():
            load_g(c + ahead).start()

        load_a(c + 1).start()
        return carry

    ahead = min(3, n_groups - 1)
    lax.fori_loop(0, ahead, pack_g, 0)
    for c in range(ahead + 1, n_groups):
        load_a(c).start()
    load_x.start()

    def conv_tile(src, wm, b, q):
        tile = jnp.concatenate([src[pl.ds(2 * b, 4), 2 * q + s].reshape(256, 128) for s in range(2)], axis=1)
        d = jnp.dot(wm[...], tile, preferred_element_type=F32)
        outs = []
        for s in range(2):
            part = d[:, s * 128:(s + 1) * 128]
            outs.append(part[64:128] + pltpu.roll(part[0:64], 127, 1) + pltpu.roll(part[128:192], 1, 1))
        return outs

    def shifted(tiles):
        left = jnp.concatenate([pltpu.roll(t, 1, 1) for t in tiles], axis=1)
        right = jnp.concatenate([pltpu.roll(t, 127, 1) for t in tiles], axis=1)
        return jnp.concatenate([left, jnp.concatenate(tiles, axis=1), right], axis=0)

    def kgrad(tiles, gref, b):
        rhs = jnp.concatenate([gref[pl.ds(2 * b, 4), j].reshape(256, 128) for j in range(8)], axis=1)
        return lax.dot_general(shifted(tiles), rhs, (((1,), (1,)), ((), ())), preferred_element_type=F32)

    def group_blocks(g):
        return [lax.rem(4 * g + k + n_blocks - 2, n_blocks) for k in range(4)]

    def middle(i, ahead):
        if ahead:
            load_g(i + ahead).wait()

        @pl.when(i + 1 < n_groups)
        def _():
            load_a(i + 1).wait()
            g_pair(i + 1, theirs).wait_recv()

        if ahead:
            pack_rows(i + ahead)
        g = lax.rem(i + 1, n_groups)
        bsum = None
        for slot, b in enumerate(group_blocks(g)):
            tiles = [jnp.concatenate([packed(raw_a, 2 * b + r, j) for r in range(2)], axis=0) for j in range(8)]
            for q in range(4):
                for s, o in enumerate(conv_tile(g_all, wm_two, b, q)):
                    j = 2 * q + s
                    m = jnp.where(tiles[j].astype(F32) > 0, o, 0.0)
                    bsum = m if bsum is None else bsum + m
                    z = m.astype(BF16)
                    for r in range(2):
                        z_all[2 * b + 1 + r, j, mine] = z[r * 32:(r + 1) * 32]
            acc[slot % 4] += kgrad(tiles, g_all, b)
        bacc[...] += bsum
        if ahead:
            g_pair(i + ahead, mine).start()

            @pl.when(i + ahead == n_groups - 1)
            def _():
                for rel in range(2):
                    halo(g_all, 0, rel, gh_send, gh_recv).start()

        for part in range(2):
            z_pair(g, part, mine).start()

    for i, wm in ((1, wm_two), (0, wm_one)):
        load_w[i].wait()
        for kw in range(3):
            for r in range(2):
                blocks = []
                for rr in range(4):
                    kh = r + 2 - rr
                    blocks.append(w_raw[i, kh, kw] if 0 <= kh < 3 else jnp.zeros((32, 64), BF16))
                wm[pl.ds(kw * 64 + r * 32, 32), :] = jnp.concatenate(blocks, axis=1)
    load_a(0).wait()
    g_pair(0, theirs).wait_recv()

    def middle_pack(i, carry):
        middle(i, ahead)
        return carry

    def middle_plain(i, carry):
        @pl.when(i == n_groups - 1)
        def _():
            halo_finish(g_all, gh_send, gh_recv)

        middle(i, 0)
        return carry

    lax.fori_loop(0, n_groups - ahead, middle_pack, 0)
    lax.fori_loop(n_groups - ahead, n_groups, middle_plain, 0)
    for up in range(2):
        for rel in range(2):
            halo(z_all, up, rel, zh_send, zh_recv).start()

    def reduce_copy(i, p, t, k, slot):
        axis = (p + t) % 3
        ref = red.at[i, p, t, slot, pl.ds(0, 56 if i == 0 and t == 0 else 48)]
        return pltpu.make_async_remote_copy(src_ref=ref, dst_ref=ref, send_sem=ar_send.at[i, p, t, k - 1], recv_sem=ar_recv.at[i, p, t, k - 1],
                                            device_id={"sp": ring_peer(axis, k), "tp": tp}, device_id_type=MESH)

    def reduce_start(i, p):
        for t in range(3):
            for k in (2, 1, 3)[:side - 1] if side > 2 else (1,):
                reduce_copy(i, p, t, k, coords[(p + t) % 3]).start()

    def reduce_begin(i):
        for t in range(3):
            top = acc[0, pl.ds(t * 64, 32), :]
            low = acc[0, pl.ds(t * 64 + 32, 32), :]
            for slot in range(1, 4):
                top = top + acc[slot, pl.ds(t * 64, 32), :]
                low = low + acc[slot, pl.ds(t * 64 + 32, 32), :]
            e = top[:, 0:192] + low[:, 64:256]
            red[i, 0, t, coords[t], pl.ds(0, 32)] = e[:, 0:128]
            red[i, 0, t, coords[t], pl.ds(32, 16)] = jnp.concatenate([e[0:16, 128:192], e[16:32, 128:192]], axis=1)
            if i == 0 and t == 0:
                both = bacc[0:32, :] + bacc[32:64, :]
                col = jnp.sum(both, axis=1, keepdims=True)
                row = jnp.broadcast_to(col, (32, 128)).T[0:8]
                red[i, 0, t, coords[t], pl.ds(48, 8)] = jnp.concatenate([row, jnp.zeros((8, 96), F32)], axis=1)
        reduce_start(i, 0)

    def reduce_step(i, p):
        for t in range(3):
            n = 56 if i == 0 and t == 0 else 48
            axis = (p + t) % 3
            me = coords[axis]
            for k in range(1, side):
                reduce_copy(i, p, t, k, lax.rem(me - k + side, side)).wait_recv()
            total = red[i, p, t, 0, pl.ds(0, n)]
            for c in range(1, side):
                total = total + red[i, p, t, c, pl.ds(0, n)]
            if p < 2:
                red[i, p + 1, t, coords[(p + 1 + t) % 3], pl.ds(0, n)] = total
            else:
                out = (dw_one, dw_two)[i]
                out[2, t] = total[0:32, 0:64]
                out[1, t] = total[0:32, 64:128]
                out[0, t] = jnp.concatenate([total[32:48, 0:64], total[32:48, 64:128]], axis=0)
                if i == 0 and t == 0:
                    dbias[...] = total[48:49, 0:32]
        if p < 2:
            reduce_start(i, p + 1)

    reduce_begin(1)
    acc[...] = jnp.zeros_like(acc)

    def z_wait(g):
        for part in range(2):
            z_pair(g, part, theirs).wait_recv()

    def tail_grad(i, carry):
        @pl.when((i > 0) & (i < n_groups // 2 - 1))
        def _():
            for k in range(2):
                z_wait(lax.rem(2 * i + 3 + k, n_groups))

        @pl.when(i == n_groups // 2 - 1)
        def _():
            halo_finish(z_all, zh_send, zh_recv)

        dw = None
        for k in range(2):
            for b in group_blocks(lax.rem(2 * i + 2 + k, n_groups)):
                tiles = [jnp.concatenate([packed(raw_x, 2 * b + r, j) for r in range(2)], axis=0) for j in range(8)]
                part = kgrad(tiles, z_all, b)
                dw = part if dw is None else dw + part
        acc[0] += dw
        return carry

    load_x.wait()
    for g in range(1, 5):
        z_wait(g % n_groups)
    lax.fori_loop(0, n_groups // 2 - 1, tail_grad, 0)
    reduce_step(1, 0)
    lax.fori_loop(n_groups // 2 - 1, n_groups // 2, tail_grad, 0)
    reduce_begin(0)

    def last(c, carry):
        for k in range(4):
            b = 4 * c + k
            for q in range(4):
                for s, o in enumerate(conv_tile(z_all, wm_one, b, q)):
                    j = 2 * q + s
                    for r in range(2):
                        gy = g_all[2 * b + 1 + r, j, mine].astype(F32)
                        v = (gy + o[r * 32:(r + 1) * 32]).astype(BF16)
                        dx_hbm[j, 2 * b + r] = v[:, 0:56]
                        dx_hbm[j + 8, 2 * b + r] = v[:, 64:120]
        return carry

    def reduce_sent(i, p):
        for t in range(3):
            for k in range(1, side):
                reduce_copy(i, p, t, k, coords[(p + t) % 3]).wait_send()

    third = max(n_groups // 3, 1)
    lax.fori_loop(0, third, last, 0)
    reduce_step(1, 1)
    for p in range(2):
        reduce_sent(1, p)
    reduce_step(0, 0)
    lax.fori_loop(third, min(2 * third, n_groups), last, 0)
    reduce_step(1, 2)
    reduce_sent(1, 2)
    reduce_sent(0, 0)
    reduce_step(0, 1)
    lax.fori_loop(min(2 * third, n_groups), n_groups, last, 0)
    for c in range(n_groups):
        g_pair(c, mine).wait_send()
        for part in range(2):
            z_pair(c, part, mine).wait_send()
    for up in range(2):
        for rel in range(2):
            halo(g_all, up, rel, gh_send, gh_recv).wait_send()
            halo(z_all, up, rel, zh_send, zh_recv).wait_send()
    reduce_sent(0, 1)
    reduce_sent(0, 2)
    reduce_step(0, 2)


def write_out(*refs):
    sems = refs[8]
    copies = [pltpu.make_async_copy(refs[i], refs[4 + i], sems.at[i]) for i in range(4)]
    for copy in copies:
        copy.start()
    for copy in copies:
        copy.wait()


def solution(mesh):
    side = round(mesh.shape["sp"] ** (1 / 3))

    def local_step(x_in, act_saved, w_one, w_two, d_out):
        swap = lambda v: jnp.transpose(v, (0, 1, 3, 2))
        imgs, rows, width, ch = x_in.shape
        n_groups = rows // 8
        raw = pltpu.VMEM((imgs, rows, ch, width), BF16)
        full = pltpu.VMEM((rows + 2, 8, 64, 128), BF16)
        dma = pltpu.SemaphoreType.DMA
        vmem = pl.BlockSpec(memory_space=pltpu.VMEM)
        hbm = pl.BlockSpec(memory_space=pltpu.HBM)
        dx, dw_one, dw_two, dbias = pl.pallas_call(
            functools.partial(body, side, rows),
            out_shape=(
                pltpu.VMEM((imgs, rows, ch, width), BF16),
                pltpu.VMEM((3, 3, 32, 64), F32),
                pltpu.VMEM((3, 3, 32, 64), F32),
                pltpu.VMEM((1, 32), F32),
            ),
            in_specs=[hbm, hbm, hbm, hbm, hbm],
            out_specs=(vmem, vmem, vmem, vmem),
            scratch_shapes=[
                raw, raw, raw, full, full, pltpu.VMEM((2, 3, 3, 32, 64), BF16),
                pltpu.VMEM((192, 256), BF16), pltpu.VMEM((192, 256), BF16),
                pltpu.VMEM((4, 192, 256), F32), pltpu.VMEM((64, 128), F32),
                pltpu.VMEM((2, 3, 3, side, 56, 128), F32),
                dma((n_groups,)), dma((n_groups,)), dma, dma((2,)),
                dma((n_groups,)), dma((n_groups,)), dma((2, 2)), dma((2, 2)),
                dma((n_groups, 2)), dma((n_groups, 2)), dma((2, 2)), dma((2, 2)),
                dma((2, 3, 3, side - 1)), dma((2, 3, 3, side - 1)),
            ],
            compiler_params=pltpu.CompilerParams(collective_id=0, has_side_effects=True, vmem_limit_bytes=46 * 1024 * 1024),
            name="resblock_bwd",
        )(*(pltpu.with_memory_space_constraint(v, pltpu.HBM) for v in (swap(x_in), swap(act_saved), swap(d_out), w_one, w_two)))
        results = (dx, dw_one, dw_two, dbias)
        dx, dw_one, dw_two, dbias = pl.pallas_call(
            write_out,
            out_shape=tuple(jax.ShapeDtypeStruct(v.shape, v.dtype) for v in results),
            in_specs=[vmem] * 4,
            out_specs=(hbm,) * 4,
            scratch_shapes=[dma((4,))],
            compiler_params=pltpu.CompilerParams(vmem_limit_bytes=1024 * 1024),
            name="write_out",
        )(*results)
        return swap(dx), dw_one, dw_two, dbias.reshape(32)

    act_spec = P("dp", "sp", None, "tp")
    kern_spec = P(None, None, "tp", None)
    grad_spec = P("dp", None, "tp", None)
    return jax.shard_map(local_step, mesh=mesh, in_specs=(act_spec, act_spec, kern_spec, kern_spec, act_spec),
                         out_specs=(act_spec, grad_spec, grad_spec, P(("dp", "tp"))), check_vma=False)
```

```python
import functools

import jax
import jax.numpy as jnp
from jax import lax
from jax.experimental import pallas as pl
from jax.experimental.pallas import tpu as pltpu
from jax.sharding import PartitionSpec as P

MESH = pl.DeviceIdType.MESH
BF16 = jnp.bfloat16
F32 = jnp.float32


def body(side, rows, x_hbm, a_hbm, g_hbm, w_one, w_two, dx_hbm, dw_one, dw_two, dbias,
         raw_g, raw_a, raw_x, g_all, z_all, w_raw, wm_one, wm_two, acc, bacc, red,
         g_sem, a_sem, x_sem, w_sem, gx_send, gx_recv, gh_send, gh_recv, zx_send, zx_recv, zh_send, zh_recv,
         ar_send, ar_recv):
    sp = lax.axis_index("sp")
    tp = lax.axis_index("tp")
    row_devs = side * side * side
    n_groups = rows // 8
    n_blocks = rows // 2
    coords = (lax.rem(sp, side), lax.rem(lax.div(sp, side), side), lax.div(sp, side * side))
    strides = (1, side, side * side)
    nxt = lax.rem(sp + 1, row_devs)
    prv = lax.rem(sp + row_devs - 1, row_devs)
    other = 1 - tp
    mine = pl.ds(pl.multiple_of(tp * 32, 32), 32)
    theirs = pl.ds(pl.multiple_of(other * 32, 32), 32)

    def ring_peer(axis, k):
        me = coords[axis]
        return sp + (lax.rem(me + k, side) - me) * strides[axis]

    def load(hbm, raw, sem, c):
        part = pl.ds(c * 8, 8)
        return pltpu.make_async_copy(hbm.at[:, part], raw.at[:, part], sem.at[c])

    def load_g(c):
        return load(g_hbm, raw_g, g_sem, c)

    def load_a(c):
        return load(a_hbm, raw_a, a_sem, c)

    load_x = pltpu.make_async_copy(x_hbm, raw_x, x_sem)
    load_w = [pltpu.make_async_copy(w, w_raw.at[i], w_sem.at[i]) for i, w in enumerate((w_one, w_two))]

    load_g(0).start()
    for w in load_w:
        w.start()
    for c in range(1, 4):
        load_g(c).start()
    load_a(0).start()

    barrier = pltpu.get_barrier_semaphore()
    targets = [(sp, other), (nxt, tp), (nxt, other), (prv, tp), (prv, other)]
    for axis in range(3):
        for k in range(1, side):
            targets.append((ring_peer(axis, k), tp))
    for s, t in targets:
        pl.semaphore_signal(barrier, inc=1, device_id={"sp": s, "tp": t}, device_id_type=MESH)

    bacc[...] = jnp.zeros_like(bacc)
    acc[...] = jnp.zeros_like(acc)

    def packed(raw, h, j):
        gap = jnp.zeros((32, 8), BF16)
        return jnp.concatenate([raw[j, h], gap, raw[j + 8, h], gap], axis=1)

    def remote(ref, lo, n, sl, send, recv):
        part = ref.at[pl.ds(lo, n), :, sl]
        return pltpu.make_async_remote_copy(src_ref=part, dst_ref=part, send_sem=send, recv_sem=recv,
                                            device_id={"sp": sp, "tp": other}, device_id_type=MESH)

    def halo(ref, up, rel, send, recv):
        src_row, dst_row, dev = (rows, 0, nxt) if up == 0 else (1, rows + 1, prv)
        return pltpu.make_async_remote_copy(
            src_ref=ref.at[src_row, :, mine], dst_ref=ref.at[dst_row, :, mine], send_sem=send.at[up, rel], recv_sem=recv.at[up, rel],
            device_id={"sp": dev, "tp": tp if rel == 0 else other}, device_id_type=MESH)

    def halo_finish(ref, send, recv):
        for up in range(2):
            for rel in range(2):
                dst_row, dev = (0, prv) if up == 0 else (rows + 1, nxt)
                part = ref.at[dst_row, :, mine if rel == 0 else theirs]
                pltpu.make_async_remote_copy(
                    src_ref=part, dst_ref=part, send_sem=send.at[up, rel], recv_sem=recv.at[up, rel],
                    device_id={"sp": dev, "tp": tp if rel == 0 else other}, device_id_type=MESH).wait_recv()

        @pl.when(sp == 0)
        def _():
            ref[0] = jnp.zeros((8, 64, 128), BF16)

        @pl.when(sp == row_devs - 1)
        def _():
            ref[rows + 1] = jnp.zeros((8, 64, 128), BF16)

    def g_pair(c, sl):
        return remote(g_all, c * 8 + 1, 8, sl, gx_send.at[c], gx_recv.at[c])

    def z_pair(g, part, sl):
        lo = lax.rem(8 * g + part * 4 + rows - 4, rows) + 1
        return remote(z_all, lo, 4, sl, zx_send.at[g, part], zx_recv.at[g, part])

    pl.semaphore_wait(barrier, len(targets))

    def pack_rows(c):
        for h in range(8):
            for j in range(8):
                g_all[c * 8 + h + 1, j, mine] = packed(raw_g, c * 8 + h, j)

    def pack_g(c, carry):
        load_g(c).wait()
        pack_rows(c)

        @pl.when(c == 0)
        def _():
            for rel in range(2):
                halo(g_all, 1, rel, gh_send, gh_recv).start()

        g_pair(c, mine).start()

        @pl.when(c == 0)
        def _():
            load_a(1).start()

        @pl.when((c > 0) & (c < 3))
        def _():
            load_g(c + 3).start()

        @pl.when(c >= 2)
        def _():
            load_a(c).start()
        return carry

    ahead = 4
    lax.fori_loop(0, ahead, pack_g, 0)
    for c in range(ahead, n_groups):
        load_a(c).start()
    load_x.start()

    def conv_tile(src, wm, b, q):
        tile = jnp.concatenate([src[pl.ds(2 * b, 4), 2 * q + s].reshape(256, 128) for s in range(2)], axis=1)
        d = jnp.dot(wm[...], tile, preferred_element_type=F32)
        outs = []
        for s in range(2):
            part = d[:, s * 128:(s + 1) * 128]
            outs.append(part[64:128] + pltpu.roll(part[0:64], 127, 1) + pltpu.roll(part[128:192], 1, 1))
        return outs

    def shifted(tiles):
        left = jnp.concatenate([pltpu.roll(t, 1, 1) for t in tiles], axis=1)
        right = jnp.concatenate([pltpu.roll(t, 127, 1) for t in tiles], axis=1)
        return jnp.concatenate([left, jnp.concatenate(tiles, axis=1), right], axis=0)

    def kgrad(tiles, gref, b):
        rhs = jnp.concatenate([gref[pl.ds(2 * b, 4), j].reshape(256, 128) for j in range(8)], axis=1)
        return lax.dot_general(shifted(tiles), rhs, (((1,), (1,)), ((), ())), preferred_element_type=F32)

    def group_blocks(g):
        return [lax.rem(4 * g + k + n_blocks - 2, n_blocks) for k in range(4)]

    def middle(groups, late):
        for c in late:
            load_g(c).wait()
            pack_rows(c)
        bsum = None
        for at, g in enumerate(groups):
            for k, b in enumerate(group_blocks(g)):
                slot = 4 * at + k
                tiles = [jnp.concatenate([packed(raw_a, 2 * b + r, j) for r in range(2)], axis=0) for j in range(8)]
                for q in range(4):
                    for s, o in enumerate(conv_tile(g_all, wm_two, b, q)):
                        j = 2 * q + s
                        m = jnp.where(tiles[j].astype(F32) > 0, o, 0.0)
                        bsum = m if bsum is None else bsum + m
                        z = m.astype(BF16)
                        for r in range(2):
                            z_all[2 * b + 1 + r, j, mine] = z[r * 32:(r + 1) * 32]
                acc[slot % 4] += kgrad(tiles, g_all, b)
        bacc[...] += bsum
        for c in late:
            g_pair(c, mine).start()
        for g in groups:
            for part in range(2):
                z_pair(g, part, mine).start()

    for i, wm in ((1, wm_two), (0, wm_one)):
        load_w[i].wait()
        for kw in range(3):
            for r in range(2):
                blocks = []
                for rr in range(4):
                    kh = r + 2 - rr
                    blocks.append(w_raw[i, kh, kw] if 0 <= kh < 3 else jnp.zeros((32, 64), BF16))
                wm[pl.ds(kw * 64 + r * 32, 32), :] = jnp.concatenate(blocks, axis=1)
    for c in range(2):
        load_a(c).wait()
        g_pair(c, theirs).wait_recv()
    middle([1], range(ahead, n_groups))
    for rel in range(2):
        halo(g_all, 0, rel, gh_send, gh_recv).start()

    def middle_pair(i, carry):
        for k in range(2):
            load_a(2 * i + 2 + k).wait()
            g_pair(2 * i + 2 + k, theirs).wait_recv()
        middle([2 * i + 2, 2 * i + 3], ())
        return carry

    lax.fori_loop(0, n_groups // 2 - 1, middle_pair, 0)
    halo_finish(g_all, gh_send, gh_recv)
    middle([0], ())
    for up in range(2):
        for rel in range(2):
            halo(z_all, up, rel, zh_send, zh_recv).start()

    def reduce_copy(i, p, t, k, slot):
        axis = (p + t) % 3
        ref = red.at[i, p, t, slot, pl.ds(0, 56 if i == 0 and t == 0 else 48)]
        return pltpu.make_async_remote_copy(src_ref=ref, dst_ref=ref, send_sem=ar_send.at[i, p, t, k - 1], recv_sem=ar_recv.at[i, p, t, k - 1],
                                            device_id={"sp": ring_peer(axis, k), "tp": tp}, device_id_type=MESH)

    def reduce_start(i, p):
        for t in range(3):
            for k in (2, 1, 3)[:side - 1] if side > 2 else (1,):
                reduce_copy(i, p, t, k, coords[(p + t) % 3]).start()

    def reduce_begin(i):
        for t in range(3):
            top = acc[0, pl.ds(t * 64, 32), :]
            low = acc[0, pl.ds(t * 64 + 32, 32), :]
            for slot in range(1, 4):
                top = top + acc[slot, pl.ds(t * 64, 32), :]
                low = low + acc[slot, pl.ds(t * 64 + 32, 32), :]
            e = top[:, 0:192] + low[:, 64:256]
            red[i, 0, t, coords[t], pl.ds(0, 32)] = e[:, 0:128]
            red[i, 0, t, coords[t], pl.ds(32, 16)] = jnp.concatenate([e[0:16, 128:192], e[16:32, 128:192]], axis=1)
            if i == 0 and t == 0:
                both = bacc[0:32, :] + bacc[32:64, :]
                col = jnp.sum(both, axis=1, keepdims=True)
                row = jnp.broadcast_to(col, (32, 128)).T[0:8]
                red[i, 0, t, coords[t], pl.ds(48, 8)] = jnp.concatenate([row, jnp.zeros((8, 96), F32)], axis=1)
        reduce_start(i, 0)

    def reduce_step(i, p):
        for t in range(3):
            n = 56 if i == 0 and t == 0 else 48
            axis = (p + t) % 3
            me = coords[axis]
            for k in range(1, side):
                reduce_copy(i, p, t, k, lax.rem(me - k + side, side)).wait_recv()
            total = red[i, p, t, 0, pl.ds(0, n)]
            for c in range(1, side):
                total = total + red[i, p, t, c, pl.ds(0, n)]
            if p < 2:
                red[i, p + 1, t, coords[(p + 1 + t) % 3], pl.ds(0, n)] = total
            else:
                out = (dw_one, dw_two)[i]
                out[2, t] = total[0:32, 0:64]
                out[1, t] = total[0:32, 64:128]
                out[0, t] = jnp.concatenate([total[32:48, 0:64], total[32:48, 64:128]], axis=0)
                if i == 0 and t == 0:
                    dbias[...] = total[48:49, 0:32]
        if p < 2:
            reduce_start(i, p + 1)

    reduce_begin(1)
    acc[...] = jnp.zeros_like(acc)

    def z_wait(g):
        for part in range(2):
            z_pair(g, part, theirs).wait_recv()

    def tail_grad(i, carry):
        @pl.when((i > 0) & (i < n_groups // 2 - 1))
        def _():
            for k in range(2):
                z_wait(lax.rem(2 * i + 3 + k, n_groups))

        @pl.when(i == n_groups // 2 - 1)
        def _():
            halo_finish(z_all, zh_send, zh_recv)

        dw = None
        for k in range(2):
            for b in group_blocks(lax.rem(2 * i + 2 + k, n_groups)):
                tiles = [jnp.concatenate([packed(raw_x, 2 * b + r, j) for r in range(2)], axis=0) for j in range(8)]
                part = kgrad(tiles, z_all, b)
                dw = part if dw is None else dw + part
        acc[0] += dw
        return carry

    load_x.wait()
    for g in range(1, 5):
        z_wait(g % n_groups)
    lax.fori_loop(0, n_groups // 2, tail_grad, 0)
    reduce_begin(0)
    reduce_step(1, 0)

    def last(c, carry):
        for k in range(4):
            b = 4 * c + k
            for q in range(4):
                for s, o in enumerate(conv_tile(z_all, wm_one, b, q)):
                    j = 2 * q + s
                    for r in range(2):
                        gy = g_all[2 * b + 1 + r, j, mine].astype(F32)
                        v = (gy + o[r * 32:(r + 1) * 32]).astype(BF16)
                        dx_hbm[j, 2 * b + r] = v[:, 0:56]
                        dx_hbm[j + 8, 2 * b + r] = v[:, 64:120]
        return carry

    def reduce_sent(i, p):
        for t in range(3):
            for k in range(1, side):
                reduce_copy(i, p, t, k, coords[(p + t) % 3]).wait_send()

    third = max(n_groups // 3, 1)
    lax.fori_loop(0, third, last, 0)
    reduce_step(0, 0)
    reduce_step(1, 1)
    for p in range(2):
        reduce_sent(1, p)
    lax.fori_loop(third, min(2 * third, n_groups), last, 0)
    reduce_step(0, 1)
    reduce_step(1, 2)
    reduce_sent(1, 2)
    reduce_sent(0, 0)
    lax.fori_loop(min(2 * third, n_groups), n_groups, last, 0)
    for c in range(n_groups):
        g_pair(c, mine).wait_send()
        for part in range(2):
            z_pair(c, part, mine).wait_send()
    for up in range(2):
        for rel in range(2):
            halo(g_all, up, rel, gh_send, gh_recv).wait_send()
            halo(z_all, up, rel, zh_send, zh_recv).wait_send()
    reduce_sent(0, 1)
    reduce_sent(0, 2)
    reduce_step(0, 2)


def write_out(*refs):
    sems = refs[8]
    copies = [pltpu.make_async_copy(refs[i], refs[4 + i], sems.at[i]) for i in range(4)]
    for copy in copies:
        copy.start()
    for copy in copies:
        copy.wait()


def solution(mesh):
    side = round(mesh.shape["sp"] ** (1 / 3))

    def local_step(x_in, act_saved, w_one, w_two, d_out):
        swap = lambda v: jnp.transpose(v, (0, 1, 3, 2))
        imgs, rows, width, ch = x_in.shape
        n_groups = rows // 8
        raw = pltpu.VMEM((imgs, rows, ch, width), BF16)
        full = pltpu.VMEM((rows + 2, 8, 64, 128), BF16)
        dma = pltpu.SemaphoreType.DMA
        vmem = pl.BlockSpec(memory_space=pltpu.VMEM)
        hbm = pl.BlockSpec(memory_space=pltpu.HBM)
        dx, dw_one, dw_two, dbias = pl.pallas_call(
            functools.partial(body, side, rows),
            out_shape=(
                pltpu.VMEM((imgs, rows, ch, width), BF16),
                pltpu.VMEM((3, 3, 32, 64), F32),
                pltpu.VMEM((3, 3, 32, 64), F32),
                pltpu.VMEM((1, 32), F32),
            ),
            in_specs=[hbm, hbm, hbm, hbm, hbm],
            out_specs=(vmem, vmem, vmem, vmem),
            scratch_shapes=[
                raw, raw, raw, full, full, pltpu.VMEM((2, 3, 3, 32, 64), BF16),
                pltpu.VMEM((192, 256), BF16), pltpu.VMEM((192, 256), BF16),
                pltpu.VMEM((4, 192, 256), F32), pltpu.VMEM((64, 128), F32),
                pltpu.VMEM((2, 3, 3, side, 56, 128), F32),
                dma((n_groups,)), dma((n_groups,)), dma, dma((2,)),
                dma((n_groups,)), dma((n_groups,)), dma((2, 2)), dma((2, 2)),
                dma((n_groups, 2)), dma((n_groups, 2)), dma((2, 2)), dma((2, 2)),
                dma((2, 3, 3, side - 1)), dma((2, 3, 3, side - 1)),
            ],
            compiler_params=pltpu.CompilerParams(collective_id=0, has_side_effects=True, vmem_limit_bytes=46 * 1024 * 1024),
            name="resblock_bwd",
        )(*(pltpu.with_memory_space_constraint(v, pltpu.HBM) for v in (swap(x_in), swap(act_saved), swap(d_out), w_one, w_two)))
        results = (dx, dw_one, dw_two, dbias)
        dx, dw_one, dw_two, dbias = pl.pallas_call(
            write_out,
            out_shape=tuple(jax.ShapeDtypeStruct(v.shape, v.dtype) for v in results),
            in_specs=[vmem] * 4,
            out_specs=(hbm,) * 4,
            scratch_shapes=[dma((4,))],
            compiler_params=pltpu.CompilerParams(vmem_limit_bytes=1024 * 1024),
            name="write_out",
        )(*results)
        return swap(dx), dw_one, dw_two, dbias.reshape(32)

    act_spec = P("dp", "sp", None, "tp")
    kern_spec = P(None, None, "tp", None)
    grad_spec = P("dp", None, "tp", None)
    return jax.shard_map(local_step, mesh=mesh, in_specs=(act_spec, act_spec, kern_spec, kern_spec, act_spec),
                         out_specs=(act_spec, grad_spec, grad_spec, P(("dp", "tp"))), check_vma=False)
```

```python
import functools

import jax
import jax.numpy as jnp
from jax import lax
from jax.experimental import pallas as pl
from jax.experimental.pallas import tpu as pltpu
from jax.sharding import PartitionSpec as P

MESH = pl.DeviceIdType.MESH
BF16 = jnp.bfloat16
F32 = jnp.float32


def body(side, rows, x_hbm, a_hbm, g_hbm, w_one, w_two, dx_hbm, dw_one, dw_two, dbias,
         raw_g, raw_a, raw_x, g_all, z_all, w_raw, wm_one, wm_two, acc, bacc, red,
         g_sem, a_sem, x_sem, w_sem, gx_send, gx_recv, gh_send, gh_recv, zx_send, zx_recv, zh_send, zh_recv,
         ar_send, ar_recv):
    sp = lax.axis_index("sp")
    tp = lax.axis_index("tp")
    row_devs = side * side * side
    n_groups = rows // 8
    n_blocks = rows // 2
    coords = (lax.rem(sp, side), lax.rem(lax.div(sp, side), side), lax.div(sp, side * side))
    strides = (1, side, side * side)
    nxt = lax.rem(sp + 1, row_devs)
    prv = lax.rem(sp + row_devs - 1, row_devs)
    other = 1 - tp
    mine = pl.ds(pl.multiple_of(tp * 32, 32), 32)
    theirs = pl.ds(pl.multiple_of(other * 32, 32), 32)

    def ring_peer(axis, k):
        me = coords[axis]
        return sp + (lax.rem(me + k, side) - me) * strides[axis]

    def load(hbm, raw, sem, c):
        part = pl.ds(c * 8, 8)
        return pltpu.make_async_copy(hbm.at[:, part], raw.at[:, part], sem.at[c])

    def load_g(c):
        return load(g_hbm, raw_g, g_sem, c)

    def load_a(c):
        return load(a_hbm, raw_a, a_sem, c)

    load_x = pltpu.make_async_copy(x_hbm, raw_x, x_sem)
    load_w = [pltpu.make_async_copy(w, w_raw.at[i], w_sem.at[i]) for i, w in enumerate((w_one, w_two))]

    load_g(0).start()
    for w in load_w:
        w.start()
    for c in range(1, 4):
        load_g(c).start()
    load_a(0).start()

    barrier = pltpu.get_barrier_semaphore()
    targets = [(sp, other), (nxt, tp), (nxt, other), (prv, tp), (prv, other)]
    for axis in range(3):
        for k in range(1, side):
            targets.append((ring_peer(axis, k), tp))
    for s, t in targets:
        pl.semaphore_signal(barrier, inc=1, device_id={"sp": s, "tp": t}, device_id_type=MESH)

    bacc[...] = jnp.zeros_like(bacc)
    acc[...] = jnp.zeros_like(acc)

    def packed(raw, h, j):
        gap = jnp.zeros((32, 8), BF16)
        return jnp.concatenate([raw[j, h], gap, raw[j + 8, h], gap], axis=1)

    def remote(ref, lo, n, sl, send, recv):
        part = ref.at[pl.ds(lo, n), :, sl]
        return pltpu.make_async_remote_copy(src_ref=part, dst_ref=part, send_sem=send, recv_sem=recv,
                                            device_id={"sp": sp, "tp": other}, device_id_type=MESH)

    def halo(ref, up, rel, send, recv):
        src_row, dst_row, dev = (rows, 0, nxt) if up == 0 else (1, rows + 1, prv)
        return pltpu.make_async_remote_copy(
            src_ref=ref.at[src_row, :, mine], dst_ref=ref.at[dst_row, :, mine], send_sem=send.at[up, rel], recv_sem=recv.at[up, rel],
            device_id={"sp": dev, "tp": tp if rel == 0 else other}, device_id_type=MESH)

    def halo_finish(ref, send, recv):
        for up in range(2):
            for rel in range(2):
                dst_row, dev = (0, prv) if up == 0 else (rows + 1, nxt)
                part = ref.at[dst_row, :, mine if rel == 0 else theirs]
                pltpu.make_async_remote_copy(
                    src_ref=part, dst_ref=part, send_sem=send.at[up, rel], recv_sem=recv.at[up, rel],
                    device_id={"sp": dev, "tp": tp if rel == 0 else other}, device_id_type=MESH).wait_recv()

        @pl.when(sp == 0)
        def _():
            ref[0] = jnp.zeros((8, 64, 128), BF16)

        @pl.when(sp == row_devs - 1)
        def _():
            ref[rows + 1] = jnp.zeros((8, 64, 128), BF16)

    def g_pair(c, sl):
        return remote(g_all, c * 8 + 1, 8, sl, gx_send.at[c], gx_recv.at[c])

    def z_pair(g, part, sl):
        lo = lax.rem(8 * g + part * 4 + rows - 4, rows) + 1
        return remote(z_all, lo, 4, sl, zx_send.at[g, part], zx_recv.at[g, part])

    pl.semaphore_wait(barrier, len(targets))

    def pack_rows(c):
        for h in range(8):
            for j in range(8):
                g_all[c * 8 + h + 1, j, mine] = packed(raw_g, c * 8 + h, j)

    def pack_g(c, carry):
        load_g(c).wait()
        pack_rows(c)

        @pl.when(c == 0)
        def _():
            for rel in range(2):
                halo(g_all, 1, rel, gh_send, gh_recv).start()

        g_pair(c, mine).start()

        @pl.when(c == 0)
        def _():
            load_a(1).start()

        @pl.when((c > 0) & (c < 3))
        def _():
            load_g(c + 3).start()

        @pl.when(c >= 2)
        def _():
            load_a(c).start()
        return carry

    ahead = 4
    lax.fori_loop(0, ahead, pack_g, 0)
    for c in range(ahead, n_groups):
        load_a(c).start()
    load_x.start()

    def conv_tile(src, wm, b, q):
        tile = jnp.concatenate([src[pl.ds(2 * b, 4), 2 * q + s].reshape(256, 128) for s in range(2)], axis=1)
        d = jnp.dot(wm[...], tile, preferred_element_type=F32)
        outs = []
        for s in range(2):
            part = d[:, s * 128:(s + 1) * 128]
            outs.append(part[64:128] + pltpu.roll(part[0:64], 127, 1) + pltpu.roll(part[128:192], 1, 1))
        return outs

    def shifted(tiles):
        left = jnp.concatenate([pltpu.roll(t, 1, 1) for t in tiles], axis=1)
        right = jnp.concatenate([pltpu.roll(t, 127, 1) for t in tiles], axis=1)
        return jnp.concatenate([left, jnp.concatenate(tiles, axis=1), right], axis=0)

    def kgrad(tiles, gref, b):
        rhs = jnp.concatenate([gref[pl.ds(2 * b, 4), j].reshape(256, 128) for j in range(8)], axis=1)
        return lax.dot_general(shifted(tiles), rhs, (((1,), (1,)), ((), ())), preferred_element_type=F32)

    def group_blocks(g):
        return [lax.rem(4 * g + k + n_blocks - 2, n_blocks) for k in range(4)]

    def middle(groups, late):
        for c in late:
            load_g(c).wait()
            pack_rows(c)
        bsum = None
        for at, g in enumerate(groups):
            for k, b in enumerate(group_blocks(g)):
                slot = 4 * at + k
                tiles = [jnp.concatenate([packed(raw_a, 2 * b + r, j) for r in range(2)], axis=0) for j in range(8)]
                for q in range(4):
                    for s, o in enumerate(conv_tile(g_all, wm_two, b, q)):
                        j = 2 * q + s
                        m = jnp.where(tiles[j].astype(F32) > 0, o, 0.0)
                        bsum = m if bsum is None else bsum + m
                        z = m.astype(BF16)
                        for r in range(2):
                            z_all[2 * b + 1 + r, j, mine] = z[r * 32:(r + 1) * 32]
                acc[slot % 4] += kgrad(tiles, g_all, b)
        bacc[...] += bsum
        for c in late:
            g_pair(c, mine).start()
        for g in groups:
            for part in range(2):
                z_pair(g, part, mine).start()

    for i, wm in ((1, wm_two), (0, wm_one)):
        load_w[i].wait()
        for kw in range(3):
            for r in range(2):
                blocks = []
                for rr in range(4):
                    kh = r + 2 - rr
                    blocks.append(w_raw[i, kh, kw] if 0 <= kh < 3 else jnp.zeros((32, 64), BF16))
                wm[pl.ds(kw * 64 + r * 32, 32), :] = jnp.concatenate(blocks, axis=1)
    for c in range(2):
        load_a(c).wait()
        g_pair(c, theirs).wait_recv()
    middle([1], range(ahead, n_groups))
    for rel in range(2):
        halo(g_all, 0, rel, gh_send, gh_recv).start()

    def middle_pair(i, carry):
        for k in range(2):
            load_a(2 * i + 2 + k).wait()
            g_pair(2 * i + 2 + k, theirs).wait_recv()
        middle([2 * i + 2, 2 * i + 3], ())
        return carry

    lax.fori_loop(0, n_groups // 2 - 1, middle_pair, 0)
    halo_finish(g_all, gh_send, gh_recv)
    middle([0], ())
    for up in range(2):
        for rel in range(2):
            halo(z_all, up, rel, zh_send, zh_recv).start()

    def reduce_copy(i, p, t, k, slot):
        axis = (p + t) % 3
        ref = red.at[i, p, t, slot, pl.ds(0, 56 if i == 0 and t == 0 else 48)]
        return pltpu.make_async_remote_copy(src_ref=ref, dst_ref=ref, send_sem=ar_send.at[i, p, t, k - 1], recv_sem=ar_recv.at[i, p, t, k - 1],
                                            device_id={"sp": ring_peer(axis, k), "tp": tp}, device_id_type=MESH)

    def reduce_start(i, p):
        for t in range(3):
            for k in (2, 1, 3)[:side - 1] if side > 2 else (1,):
                reduce_copy(i, p, t, k, coords[(p + t) % 3]).start()

    def reduce_begin(i):
        slots = 1 if i == 0 else 4
        for t in range(3):
            top = acc[0, pl.ds(t * 64, 32), :]
            low = acc[0, pl.ds(t * 64 + 32, 32), :]
            for slot in range(1, slots):
                top = top + acc[slot, pl.ds(t * 64, 32), :]
                low = low + acc[slot, pl.ds(t * 64 + 32, 32), :]
            e = top[:, 0:192] + low[:, 64:256]
            red[i, 0, t, coords[t], pl.ds(0, 32)] = e[:, 0:128]
            red[i, 0, t, coords[t], pl.ds(32, 16)] = jnp.concatenate([e[0:16, 128:192], e[16:32, 128:192]], axis=1)
        reduce_start(i, 0)

    def reduce_step(i, p):
        for t in range(3):
            n = 56 if i == 0 and t == 0 else 48
            axis = (p + t) % 3
            me = coords[axis]
            for k in range(1, side):
                reduce_copy(i, p, t, k, lax.rem(me - k + side, side)).wait_recv()
            total = red[i, p, t, 0, pl.ds(0, n)]
            for c in range(1, side):
                total = total + red[i, p, t, c, pl.ds(0, n)]
            if p < 2:
                red[i, p + 1, t, coords[(p + 1 + t) % 3], pl.ds(0, n)] = total
            else:
                out = (dw_one, dw_two)[i]
                out[2, t] = total[0:32, 0:64]
                out[1, t] = total[0:32, 64:128]
                out[0, t] = jnp.concatenate([total[32:48, 0:64], total[32:48, 64:128]], axis=0)
                if i == 0 and t == 0:
                    dbias[...] = total[48:49, 0:32]
        if p < 2:
            reduce_start(i, p + 1)

    reduce_begin(1)
    acc[0] = jnp.zeros((192, 256), F32)
    col = jnp.sum(bacc[0:32, :] + bacc[32:64, :], axis=1, keepdims=True)
    row = jnp.broadcast_to(col, (32, 128)).T[0:8]
    red[0, 0, 0, coords[0], pl.ds(48, 8)] = jnp.concatenate([row, jnp.zeros((8, 96), F32)], axis=1)

    def z_wait(g):
        for part in range(2):
            z_pair(g, part, theirs).wait_recv()

    def tail_grad(i, carry):
        @pl.when((i > 0) & (i < n_groups // 2 - 1))
        def _():
            for k in range(2):
                z_wait(lax.rem(2 * i + 3 + k, n_groups))

        @pl.when(i == n_groups // 2 - 1)
        def _():
            halo_finish(z_all, zh_send, zh_recv)

        dw = None
        for k in range(2):
            for b in group_blocks(lax.rem(2 * i + 2 + k, n_groups)):
                tiles = [jnp.concatenate([packed(raw_x, 2 * b + r, j) for r in range(2)], axis=0) for j in range(8)]
                part = kgrad(tiles, z_all, b)
                dw = part if dw is None else dw + part
        acc[0] += dw
        return carry

    load_x.wait()
    for g in range(1, 5):
        z_wait(g % n_groups)
    lax.fori_loop(0, n_groups // 2, tail_grad, 0)
    reduce_begin(0)
    reduce_step(1, 0)

    def last(c, carry):
        for k in range(4):
            b = 4 * c + k
            for q in range(4):
                for s, o in enumerate(conv_tile(z_all, wm_one, b, q)):
                    j = 2 * q + s
                    for r in range(2):
                        gy = g_all[2 * b + 1 + r, j, mine].astype(F32)
                        v = (gy + o[r * 32:(r + 1) * 32]).astype(BF16)
                        dx_hbm[j, 2 * b + r] = v[:, 0:56]
                        dx_hbm[j + 8, 2 * b + r] = v[:, 64:120]
        return carry

    def reduce_sent(i, p):
        for t in range(3):
            for k in range(1, side):
                reduce_copy(i, p, t, k, coords[(p + t) % 3]).wait_send()

    third = max(n_groups // 3, 1)
    lax.fori_loop(0, third, last, 0)
    reduce_step(0, 0)
    reduce_step(1, 1)
    for p in range(2):
        reduce_sent(1, p)
    lax.fori_loop(third, min(2 * third, n_groups), last, 0)
    reduce_step(0, 1)
    reduce_step(1, 2)
    reduce_sent(1, 2)
    reduce_sent(0, 0)
    lax.fori_loop(min(2 * third, n_groups), n_groups, last, 0)
    for c in range(n_groups):
        g_pair(c, mine).wait_send()
        for part in range(2):
            z_pair(c, part, mine).wait_send()
    for up in range(2):
        for rel in range(2):
            halo(g_all, up, rel, gh_send, gh_recv).wait_send()
            halo(z_all, up, rel, zh_send, zh_recv).wait_send()
    reduce_sent(0, 1)
    reduce_sent(0, 2)
    reduce_step(0, 2)


def write_out(*refs):
    sems = refs[8]
    copies = [pltpu.make_async_copy(refs[i], refs[4 + i], sems.at[i]) for i in range(4)]
    for copy in copies:
        copy.start()
    for copy in copies:
        copy.wait()


def solution(mesh):
    side = round(mesh.shape["sp"] ** (1 / 3))

    def local_step(x_in, act_saved, w_one, w_two, d_out):
        swap = lambda v: jnp.transpose(v, (0, 1, 3, 2))
        imgs, rows, width, ch = x_in.shape
        n_groups = rows // 8
        raw = pltpu.VMEM((imgs, rows, ch, width), BF16)
        full = pltpu.VMEM((rows + 2, 8, 64, 128), BF16)
        dma = pltpu.SemaphoreType.DMA
        vmem = pl.BlockSpec(memory_space=pltpu.VMEM)
        hbm = pl.BlockSpec(memory_space=pltpu.HBM)
        dx, dw_one, dw_two, dbias = pl.pallas_call(
            functools.partial(body, side, rows),
            out_shape=(
                pltpu.VMEM((imgs, rows, ch, width), BF16),
                pltpu.VMEM((3, 3, 32, 64), F32),
                pltpu.VMEM((3, 3, 32, 64), F32),
                pltpu.VMEM((1, 32), F32),
            ),
            in_specs=[hbm, hbm, hbm, hbm, hbm],
            out_specs=(vmem, vmem, vmem, vmem),
            scratch_shapes=[
                raw, raw, raw, full, full, pltpu.VMEM((2, 3, 3, 32, 64), BF16),
                pltpu.VMEM((192, 256), BF16), pltpu.VMEM((192, 256), BF16),
                pltpu.VMEM((4, 192, 256), F32), pltpu.VMEM((64, 128), F32),
                pltpu.VMEM((2, 3, 3, side, 56, 128), F32),
                dma((n_groups,)), dma((n_groups,)), dma, dma((2,)),
                dma((n_groups,)), dma((n_groups,)), dma((2, 2)), dma((2, 2)),
                dma((n_groups, 2)), dma((n_groups, 2)), dma((2, 2)), dma((2, 2)),
                dma((2, 3, 3, side - 1)), dma((2, 3, 3, side - 1)),
            ],
            compiler_params=pltpu.CompilerParams(collective_id=0, has_side_effects=True, vmem_limit_bytes=46 * 1024 * 1024),
            name="resblock_bwd",
        )(*(pltpu.with_memory_space_constraint(v, pltpu.HBM) for v in (swap(x_in), swap(act_saved), swap(d_out), w_one, w_two)))
        results = (dx, dw_one, dw_two, dbias)
        dx, dw_one, dw_two, dbias = pl.pallas_call(
            write_out,
            out_shape=tuple(jax.ShapeDtypeStruct(v.shape, v.dtype) for v in results),
            in_specs=[vmem] * 4,
            out_specs=(hbm,) * 4,
            scratch_shapes=[dma((4,))],
            compiler_params=pltpu.CompilerParams(vmem_limit_bytes=1024 * 1024),
            name="write_out",
        )(*results)
        return swap(dx), dw_one, dw_two, dbias.reshape(32)

    act_spec = P("dp", "sp", None, "tp")
    kern_spec = P(None, None, "tp", None)
    grad_spec = P("dp", None, "tp", None)
    return jax.shard_map(local_step, mesh=mesh, in_specs=(act_spec, act_spec, kern_spec, kern_spec, act_spec),
                         out_specs=(act_spec, grad_spec, grad_spec, P(("dp", "tp"))), check_vma=False)
```

```python
import functools

import jax
import jax.numpy as jnp
from jax import lax
from jax.experimental import pallas as pl
from jax.experimental.pallas import tpu as pltpu
from jax.sharding import PartitionSpec as P

MESH = pl.DeviceIdType.MESH
BF16 = jnp.bfloat16
F32 = jnp.float32


def body(side, rows, x_hbm, a_hbm, g_hbm, w_one, w_two, dx_hbm, dw_one, dw_two, dbias,
         raw_g, raw_a, raw_x, g_all, z_all, w_raw, wm_one, wm_two, acc, bacc, red,
         g_sem, a_sem, x_sem, w_sem, gx_send, gx_recv, gh_send, gh_recv, zx_send, zx_recv, zh_send, zh_recv,
         ar_send, ar_recv):
    sp = lax.axis_index("sp")
    tp = lax.axis_index("tp")
    row_devs = side * side * side
    n_groups = rows // 8
    n_blocks = rows // 2
    coords = (lax.rem(sp, side), lax.rem(lax.div(sp, side), side), lax.div(sp, side * side))
    strides = (1, side, side * side)
    nxt = lax.rem(sp + 1, row_devs)
    prv = lax.rem(sp + row_devs - 1, row_devs)
    other = 1 - tp
    mine = pl.ds(pl.multiple_of(tp * 32, 32), 32)
    theirs = pl.ds(pl.multiple_of(other * 32, 32), 32)

    def ring_peer(axis, k):
        me = coords[axis]
        return sp + (lax.rem(me + k, side) - me) * strides[axis]

    def load(hbm, raw, sem, c):
        part = pl.ds(c * 8, 8)
        return pltpu.make_async_copy(hbm.at[:, part], raw.at[:, part], sem.at[c])

    def load_g(c):
        return load(g_hbm, raw_g, g_sem, c)

    def load_a(c):
        return load(a_hbm, raw_a, a_sem, c)

    load_x = pltpu.make_async_copy(x_hbm, raw_x, x_sem)
    load_w = [pltpu.make_async_copy(w, w_raw.at[i], w_sem.at[i]) for i, w in enumerate((w_one, w_two))]

    load_g(0).start()
    for w in load_w:
        w.start()
    for c in range(1, 4):
        load_g(c).start()
    load_a(0).start()

    barrier = pltpu.get_barrier_semaphore()
    targets = [(sp, other), (nxt, tp), (nxt, other), (prv, tp), (prv, other)]
    for axis in range(3):
        for k in range(1, side):
            targets.append((ring_peer(axis, k), tp))
    for s, t in targets:
        pl.semaphore_signal(barrier, inc=1, device_id={"sp": s, "tp": t}, device_id_type=MESH)

    bacc[...] = jnp.zeros_like(bacc)
    acc[...] = jnp.zeros_like(acc)

    def packed(raw, h, j):
        gap = jnp.zeros((32, 8), BF16)
        return jnp.concatenate([raw[j, h], gap, raw[j + 8, h], gap], axis=1)

    def remote(ref, lo, n, sl, send, recv):
        part = ref.at[pl.ds(lo, n), :, sl]
        return pltpu.make_async_remote_copy(src_ref=part, dst_ref=part, send_sem=send, recv_sem=recv,
                                            device_id={"sp": sp, "tp": other}, device_id_type=MESH)

    def halo(ref, up, rel, send, recv):
        src_row, dst_row, dev = (rows, 0, nxt) if up == 0 else (1, rows + 1, prv)
        return pltpu.make_async_remote_copy(
            src_ref=ref.at[src_row, :, mine], dst_ref=ref.at[dst_row, :, mine], send_sem=send.at[up, rel], recv_sem=recv.at[up, rel],
            device_id={"sp": dev, "tp": tp if rel == 0 else other}, device_id_type=MESH)

    def halo_finish(ref, send, recv):
        for up in range(2):
            for rel in range(2):
                dst_row, dev = (0, prv) if up == 0 else (rows + 1, nxt)
                part = ref.at[dst_row, :, mine if rel == 0 else theirs]
                pltpu.make_async_remote_copy(
                    src_ref=part, dst_ref=part, send_sem=send.at[up, rel], recv_sem=recv.at[up, rel],
                    device_id={"sp": dev, "tp": tp if rel == 0 else other}, device_id_type=MESH).wait_recv()

        @pl.when(sp == 0)
        def _():
            ref[0] = jnp.zeros((8, 64, 128), BF16)

        @pl.when(sp == row_devs - 1)
        def _():
            ref[rows + 1] = jnp.zeros((8, 64, 128), BF16)

    def g_pair(c, sl):
        return remote(g_all, c * 8 + 1, 8, sl, gx_send.at[c], gx_recv.at[c])

    def z_pair(g, part, sl):
        lo = lax.rem(8 * g + part * 4 + rows - 4, rows) + 1
        return remote(z_all, lo, 4, sl, zx_send.at[g, part], zx_recv.at[g, part])

    pl.semaphore_wait(barrier, len(targets))

    def pack_rows(c):
        for h in range(8):
            for j in range(8):
                g_all[c * 8 + h + 1, j, mine] = packed(raw_g, c * 8 + h, j)

    def pack_g(c, carry):
        load_g(c).wait()
        pack_rows(c)

        @pl.when(c == 0)
        def _():
            for rel in range(2):
                halo(g_all, 1, rel, gh_send, gh_recv).start()

        g_pair(c, mine).start()

        @pl.when(c == 0)
        def _():
            load_a(1).start()

        @pl.when((c > 0) & (c < 3))
        def _():
            load_g(c + 3).start()

        @pl.when(c >= 2)
        def _():
            load_a(c).start()
        return carry

    ahead = 4
    lax.fori_loop(0, ahead, pack_g, 0)
    for c in range(ahead, n_groups):
        load_a(c).start()
    load_x.start()

    def conv_tile(src, wm, b, q):
        tile = jnp.concatenate([src[pl.ds(2 * b, 4), 2 * q + s].reshape(256, 128) for s in range(2)], axis=1)
        d = jnp.dot(wm[...], tile, preferred_element_type=F32)
        outs = []
        for s in range(2):
            part = d[:, s * 128:(s + 1) * 128]
            outs.append(part[64:128] + pltpu.roll(part[0:64], 127, 1) + pltpu.roll(part[128:192], 1, 1))
        return outs

    def shifted(tiles):
        left = jnp.concatenate([pltpu.roll(t, 1, 1) for t in tiles], axis=1)
        right = jnp.concatenate([pltpu.roll(t, 127, 1) for t in tiles], axis=1)
        return jnp.concatenate([left, jnp.concatenate(tiles, axis=1), right], axis=0)

    def kgrad(tiles, gref, b):
        rhs = jnp.concatenate([gref[pl.ds(2 * b, 4), j].reshape(256, 128) for j in range(8)], axis=1)
        return lax.dot_general(shifted(tiles), rhs, (((1,), (1,)), ((), ())), preferred_element_type=F32)

    def group_blocks(g):
        return [lax.rem(4 * g + k + n_blocks - 2, n_blocks) for k in range(4)]

    def middle(groups, late):
        for c in late:
            load_g(c).wait()
            pack_rows(c)
        bsum = None
        for at, g in enumerate(groups):
            for k, b in enumerate(group_blocks(g)):
                slot = 4 * at + k
                tiles = [jnp.concatenate([packed(raw_a, 2 * b + r, j) for r in range(2)], axis=0) for j in range(8)]
                for q in range(4):
                    for s, o in enumerate(conv_tile(g_all, wm_two, b, q)):
                        j = 2 * q + s
                        m = jnp.where(tiles[j].astype(F32) > 0, o, 0.0)
                        bsum = m if bsum is None else bsum + m
                        z = m.astype(BF16)
                        for r in range(2):
                            z_all[2 * b + 1 + r, j, mine] = z[r * 32:(r + 1) * 32]
                acc[slot % 4] += kgrad(tiles, g_all, b)
        bacc[...] += bsum
        for c in late:
            g_pair(c, mine).start()
        for g in groups:
            for part in range(2):
                z_pair(g, part, mine).start()

    for i, wm in ((1, wm_two), (0, wm_one)):
        load_w[i].wait()
        for kw in range(3):
            for r in range(2):
                blocks = []
                for rr in range(4):
                    kh = r + 2 - rr
                    blocks.append(w_raw[i, kh, kw] if 0 <= kh < 3 else jnp.zeros((32, 64), BF16))
                wm[pl.ds(kw * 64 + r * 32, 32), :] = jnp.concatenate(blocks, axis=1)
    for c in range(2):
        load_a(c).wait()
        g_pair(c, theirs).wait_recv()
    middle([1], range(ahead, n_groups))
    for rel in range(2):
        halo(g_all, 0, rel, gh_send, gh_recv).start()

    def middle_pair(i, carry):
        for k in range(2):
            load_a(2 * i + 2 + k).wait()
            g_pair(2 * i + 2 + k, theirs).wait_recv()
        middle([2 * i + 2, 2 * i + 3], ())
        return carry

    lax.fori_loop(0, n_groups // 2 - 1, middle_pair, 0)
    halo_finish(g_all, gh_send, gh_recv)
    middle([0], ())
    for up in range(2):
        for rel in range(2):
            halo(z_all, up, rel, zh_send, zh_recv).start()

    def reduce_copy(i, p, t, k, slot):
        axis = (p + t) % 3
        ref = red.at[i, p, t, slot, pl.ds(0, 56 if i == 0 and t == 0 else 48)]
        return pltpu.make_async_remote_copy(src_ref=ref, dst_ref=ref, send_sem=ar_send.at[i, p, t, k - 1], recv_sem=ar_recv.at[i, p, t, k - 1],
                                            device_id={"sp": ring_peer(axis, k), "tp": tp}, device_id_type=MESH)

    def reduce_start(i, p, thirds=range(3)):
        for t in thirds:
            for k in (2, 1, 3)[:side - 1] if side > 2 else (1,):
                reduce_copy(i, p, t, k, coords[(p + t) % 3]).start()

    def reduce_begin(i):
        slots = 1 if i == 0 else 4
        for t in range(3):
            top = acc[0, pl.ds(t * 64, 32), :]
            low = acc[0, pl.ds(t * 64 + 32, 32), :]
            for slot in range(1, slots):
                top = top + acc[slot, pl.ds(t * 64, 32), :]
                low = low + acc[slot, pl.ds(t * 64 + 32, 32), :]
            e = top[:, 0:192] + low[:, 64:256]
            red[i, 0, t, coords[t], pl.ds(0, 32)] = e[:, 0:128]
            red[i, 0, t, coords[t], pl.ds(32, 16)] = jnp.concatenate([e[0:16, 128:192], e[16:32, 128:192]], axis=1)
        reduce_start(i, 0)

    def reduce_step(i, p):
        for t in range(3):
            n = 56 if i == 0 and t == 0 else 48
            axis = (p + t) % 3
            me = coords[axis]
            for k in range(1, side):
                reduce_copy(i, p, t, k, lax.rem(me - k + side, side)).wait_recv()
            total = red[i, p, t, 0, pl.ds(0, n)]
            for c in range(1, side):
                total = total + red[i, p, t, c, pl.ds(0, n)]
            if p < 2:
                red[i, p + 1, t, coords[(p + 1 + t) % 3], pl.ds(0, n)] = total
                if t:
                    reduce_start(i, p + 1, (t - 1,))
            else:
                out = (dw_one, dw_two)[i]
                out[2, t] = total[0:32, 0:64]
                out[1, t] = total[0:32, 64:128]
                out[0, t] = jnp.concatenate([total[32:48, 0:64], total[32:48, 64:128]], axis=0)
                if i == 0 and t == 0:
                    dbias[...] = total[48:49, 0:32]
        if p < 2:
            reduce_start(i, p + 1, (2,))

    reduce_begin(1)
    acc[0] = jnp.zeros((192, 256), F32)
    col = jnp.sum(bacc[0:32, :] + bacc[32:64, :], axis=1, keepdims=True)
    row = jnp.broadcast_to(col, (32, 128)).T[0:8]
    red[0, 0, 0, coords[0], pl.ds(48, 8)] = jnp.concatenate([row, jnp.zeros((8, 96), F32)], axis=1)

    def z_wait(g):
        for part in range(2):
            z_pair(g, part, theirs).wait_recv()

    def tail_grad(i, carry):
        @pl.when((i > 0) & (i < n_groups // 2 - 1))
        def _():
            for k in range(2):
                z_wait(lax.rem(2 * i + 3 + k, n_groups))

        @pl.when(i == n_groups // 2 - 1)
        def _():
            halo_finish(z_all, zh_send, zh_recv)

        dw = None
        for k in range(2):
            for b in group_blocks(lax.rem(2 * i + 2 + k, n_groups)):
                tiles = [jnp.concatenate([packed(raw_x, 2 * b + r, j) for r in range(2)], axis=0) for j in range(8)]
                part = kgrad(tiles, z_all, b)
                dw = part if dw is None else dw + part
        acc[0] += dw
        return carry

    load_x.wait()
    for g in range(1, 5):
        z_wait(g % n_groups)
    lax.fori_loop(0, n_groups // 2, tail_grad, 0)
    reduce_begin(0)
    reduce_step(1, 0)

    def last(c, carry):
        for k in range(4):
            b = 4 * c + k
            for q in range(4):
                for s, o in enumerate(conv_tile(z_all, wm_one, b, q)):
                    j = 2 * q + s
                    for r in range(2):
                        gy = g_all[2 * b + 1 + r, j, mine].astype(F32)
                        v = (gy + o[r * 32:(r + 1) * 32]).astype(BF16)
                        dx_hbm[j, 2 * b + r] = v[:, 0:56]
                        dx_hbm[j + 8, 2 * b + r] = v[:, 64:120]
        return carry

    def reduce_sent(i, p):
        for t in range(3):
            for k in range(1, side):
                reduce_copy(i, p, t, k, coords[(p + t) % 3]).wait_send()

    third = max(n_groups // 3, 1)
    lax.fori_loop(0, third, last, 0)
    reduce_step(0, 0)
    reduce_step(1, 1)
    for p in range(2):
        reduce_sent(1, p)
    lax.fori_loop(third, min(2 * third, n_groups), last, 0)
    reduce_step(0, 1)
    reduce_step(1, 2)
    reduce_sent(1, 2)
    reduce_sent(0, 0)
    lax.fori_loop(min(2 * third, n_groups), n_groups, last, 0)
    for c in range(n_groups):
        g_pair(c, mine).wait_send()
        for part in range(2):
            z_pair(c, part, mine).wait_send()
    for up in range(2):
        for rel in range(2):
            halo(g_all, up, rel, gh_send, gh_recv).wait_send()
            halo(z_all, up, rel, zh_send, zh_recv).wait_send()
    reduce_sent(0, 1)
    reduce_sent(0, 2)
    reduce_step(0, 2)


def write_out(*refs):
    sems = refs[8]
    copies = [pltpu.make_async_copy(refs[i], refs[4 + i], sems.at[i]) for i in range(4)]
    for copy in copies:
        copy.start()
    for copy in copies:
        copy.wait()


def solution(mesh):
    side = round(mesh.shape["sp"] ** (1 / 3))

    def local_step(x_in, act_saved, w_one, w_two, d_out):
        swap = lambda v: jnp.transpose(v, (0, 1, 3, 2))
        imgs, rows, width, ch = x_in.shape
        n_groups = rows // 8
        raw = pltpu.VMEM((imgs, rows, ch, width), BF16)
        full = pltpu.VMEM((rows + 2, 8, 64, 128), BF16)
        dma = pltpu.SemaphoreType.DMA
        vmem = pl.BlockSpec(memory_space=pltpu.VMEM)
        hbm = pl.BlockSpec(memory_space=pltpu.HBM)
        dx, dw_one, dw_two, dbias = pl.pallas_call(
            functools.partial(body, side, rows),
            out_shape=(
                pltpu.VMEM((imgs, rows, ch, width), BF16),
                pltpu.VMEM((3, 3, 32, 64), F32),
                pltpu.VMEM((3, 3, 32, 64), F32),
                pltpu.VMEM((1, 32), F32),
            ),
            in_specs=[hbm, hbm, hbm, hbm, hbm],
            out_specs=(vmem, vmem, vmem, vmem),
            scratch_shapes=[
                raw, raw, raw, full, full, pltpu.VMEM((2, 3, 3, 32, 64), BF16),
                pltpu.VMEM((192, 256), BF16), pltpu.VMEM((192, 256), BF16),
                pltpu.VMEM((4, 192, 256), F32), pltpu.VMEM((64, 128), F32),
                pltpu.VMEM((2, 3, 3, side, 56, 128), F32),
                dma((n_groups,)), dma((n_groups,)), dma, dma((2,)),
                dma((n_groups,)), dma((n_groups,)), dma((2, 2)), dma((2, 2)),
                dma((n_groups, 2)), dma((n_groups, 2)), dma((2, 2)), dma((2, 2)),
                dma((2, 3, 3, side - 1)), dma((2, 3, 3, side - 1)),
            ],
            compiler_params=pltpu.CompilerParams(collective_id=0, has_side_effects=True, vmem_limit_bytes=46 * 1024 * 1024),
            name="resblock_bwd",
        )(*(pltpu.with_memory_space_constraint(v, pltpu.HBM) for v in (swap(x_in), swap(act_saved), swap(d_out), w_one, w_two)))
        results = (dx, dw_one, dw_two, dbias)
        dx, dw_one, dw_two, dbias = pl.pallas_call(
            write_out,
            out_shape=tuple(jax.ShapeDtypeStruct(v.shape, v.dtype) for v in results),
            in_specs=[vmem] * 4,
            out_specs=(hbm,) * 4,
            scratch_shapes=[dma((4,))],
            compiler_params=pltpu.CompilerParams(vmem_limit_bytes=1024 * 1024),
            name="write_out",
        )(*results)
        return swap(dx), dw_one, dw_two, dbias.reshape(32)

    act_spec = P("dp", "sp", None, "tp")
    kern_spec = P(None, None, "tp", None)
    grad_spec = P("dp", None, "tp", None)
    return jax.shard_map(local_step, mesh=mesh, in_specs=(act_spec, act_spec, kern_spec, kern_spec, act_spec),
                         out_specs=(act_spec, grad_spec, grad_spec, P(("dp", "tp"))), check_vma=False)
```
